32 devices in a mesh: sample: 4 (over y, x), gz: 8 (over z, core).
Axes of the slice: x: 2, y: 2, z: 4, core: 2. Of those that a mesh axis runs over, the one named last changes fastest.
Arguments:
- field_now: float32 [12, 16, 160, 256], P('sample', 'gz'), parts along dimension 0, may hold values from -6 to 6
- field_before: float32 [12, 16, 160, 256], P('sample', 'gz'), parts along dimension 0, may hold values from -6 to 6
- lame_lambda: float32 [16, 640, 256], P('gz', 'sample'), parts along dimension 1, may hold values from 0.5 to 1.5
- shear_modulus: float32 [16, 640, 256], P('gz', 'sample'), parts along dimension 1, may hold values from 0.5 to 1.5
- density: float32 [16, 640, 256], P('gz', 'sample'), parts along dimension 1, may hold values from 1 to 2
- source_field: float32 [12, 16, 160, 256], P('sample', 'gz'), parts along dimension 0, may hold values from -6 to 6
- wavelet: float32 [32], P('sample'), parts along dimension 0, may hold values from -4 to 4
- prior_mean: float32 [16, 640, 256], P('gz', 'sample'), parts along dimension 1, may hold values from 0.5 to 1.5
- steps_taken: float32 [16, 16, 160, 256], P('sample', 'gz'), parts along dimension 0
- grad_change: float32 [16, 16, 160, 256], P('sample', 'gz'), parts along dimension 0, as said below
Outputs:
- field_final: float32 [12, 16, 160, 256], P('sample', 'gz'), parts along dimension 0
- gradient: float32 [16, 640, 256], P('gz', 'sample'), parts along dimension 1
- direction: float32 [16, 640, 256], P('gz', 'sample'), parts along dimension 1
The draws below stay inside these ranges and needn't reach their ends.
There are 4 independent parts, one for each index of `sample`. The reference program is written for one: setup_inputs(seed, part) draws one part's arguments, and reference() takes and returns one part's arrays. A program takes and returns all parts, laid end to end along the dimension named above; each array names one. Nothing has to cross between parts.
Inputs may be any that keep to these rules, and one draw needn't show every extreme that they name: Each entry of grad_change is 0.5 to 2 times the matching entry of steps_taken.
All inputs are finite; a program needn't handle non-finite values.
Results may differ from the reference program's by a relative error of at most 0.0003.
Values sent between devices are 32-bit elements; how exact they have to be, the bound alone decides.
A program may use at most 64 MiB of HBM per device.

```python
import math
import jax
import jax.numpy as jnp
from jax import lax

NX = 160
NY = 256
STEPS = 8
PAIRS = 4
NZ = 16


def common_model(key):
    base = jax.random.fold_in(key, 11)
    keys = jax.random.split(base, 5)
    shape = (NZ, NX, NY)
    shear = jax.random.uniform(keys[0], shape, jnp.float32, 0.5, 1.5)
    prior = jax.random.uniform(keys[1], shape, jnp.float32, 0.5, 1.5)
    levels = 1.0 + 2.0 * jnp.arange(NZ, dtype=jnp.float32) / max(NZ - 1, 1)
    noise = jax.random.normal(keys[3], (PAIRS,) + shape, jnp.float32)
    weights = jax.random.uniform(keys[2], (PAIRS, 1, 1, 1), jnp.float32, 0.5, 2.0)
    updates = levels[None, :, None, None] * (weights * (shear - prior)[None] + 0.5 * noise)
    factors = jnp.exp(jax.random.uniform(keys[4], (PAIRS,) + shape, jnp.float32, -0.6931, 0.6931))
    changes = factors * updates
    return (shear, prior, updates, changes)


def draw_shear_modulus(key, part):
    return common_model(key)[0]


def draw_prior_mean(key, part):
    return common_model(key)[1]


def draw_steps_taken(key, part):
    return common_model(key)[2]


def draw_grad_change(key, part):
    return common_model(key)[3]


def shard_levels(rng, extent, cuts, low, top_value):
    def one(dim, shards_of):
        draws = jax.random.uniform(jax.random.fold_in(jax.random.fold_in(rng, 6), dim), (shards_of,), jnp.float32, low / len(cuts), top_value / len(cuts))
        return jnp.repeat(jnp.exp(draws), extent[dim] // shards_of).reshape((-1,) + (1,) * (len(extent) - dim - 1))

    level = one(*cuts[0])
    for cut in cuts[1:]:
        level = level * one(*cut)
    return level


def gaussian(key, extent, deviation, bound, pieces=(), kind=jnp.bfloat16):
    values = jax.random.normal(key, extent, jnp.float32) * deviation
    if len(pieces) > 0:
        values = shard_levels(key, extent, pieces, -0.22, 0.18) * values
    return jnp.clip(values, min=-bound, max=bound).astype(kind)


def setup_inputs(seed: int = 0, part: int = 0) -> dict:
    arg_keys = jax.random.split(jax.random.key(seed), 11)
    part_keys = jax.random.split(jax.random.fold_in(arg_keys[10], part), 11)
    field_now = gaussian(part_keys[0], (3, NZ, NX, NY), 1.0, 6.0, ((1, 8),), jnp.float32)
    field_before = gaussian(part_keys[1], (3, NZ, NX, NY), 1.0, 6.0, ((1, 8),), jnp.float32)
    lame_lambda = jnp.clip(0.5 + 1.0 * jax.random.uniform(part_keys[2], (NZ, NX, NY), jnp.float32) ** shard_levels(part_keys[2], (NZ, NX, NY), ((0, 8),), -0.2, 0.2), 0.5, 1.5)
    shear_modulus = draw_shear_modulus(jax.random.fold_in(jax.random.fold_in(arg_keys[10], part), 71), part)
    density = jnp.clip(jnp.exp(math.log(2.0) - 0.6931472 * jax.random.uniform(part_keys[4], (NZ, NX, NY), jnp.float32) ** shard_levels(part_keys[4], (NZ, NX, NY), ((0, 8),), -0.2, 0.2)), 1.0, 2.0)
    source_field = gaussian(part_keys[5], (3, NZ, NX, NY), 1.0, 6.0, ((1, 8),), jnp.float32)
    wavelet = gaussian(part_keys[6], (STEPS,), 1.0, 4.0, (), jnp.float32)
    prior_mean = draw_prior_mean(jax.random.fold_in(jax.random.fold_in(arg_keys[10], part), 71), part)
    steps_taken = draw_steps_taken(jax.random.fold_in(jax.random.fold_in(arg_keys[10], part), 71), part)
    grad_change = draw_grad_change(jax.random.fold_in(jax.random.fold_in(arg_keys[10], part), 71), part)
    return {"field_now": field_now, "field_before": field_before, "lame_lambda": lame_lambda, "shear_modulus": shear_modulus, "density": density, "source_field": source_field, "wavelet": wavelet, "prior_mean": prior_mean, "steps_taken": steps_taken, "grad_change": grad_change}


def shifted(padded, comp, offset):
    depth = padded.shape[1] - 2
    rows = padded.shape[2] - 2
    cols = padded.shape[3] - 2
    return lax.slice(padded[comp], (1 + offset[0], 1 + offset[1], 1 + offset[2]), (1 + offset[0] + depth, 1 + offset[1] + rows, 1 + offset[2] + cols))


def vec_add(first, second):
    return (first[0] + second[0], first[1] + second[1], first[2] + second[2])


def vec_neg(first):
    return (-first[0], -first[1], -first[2])


def operate(extended, lame_first, shear):
    padded = jnp.pad(extended, ((0, 0), (0, 0), (1, 1), (1, 1)))
    units = ((1, 0, 0), (0, 1, 0), (0, 0, 1))
    centre = (0, 0, 0)
    seconds = [[shifted(padded, comp, units[axis]) + shifted(padded, comp, vec_neg(units[axis])) - 2.0 * shifted(padded, comp, centre) for axis in range(3)] for comp in range(3)]

    def mixed(comp, first, second):
        plus_first = units[first]
        plus_second = units[second]
        return 0.25 * (shifted(padded, comp, vec_add(plus_first, plus_second)) - shifted(padded, comp, vec_add(plus_first, vec_neg(plus_second))) - shifted(padded, comp, vec_add(vec_neg(plus_first), plus_second)) + shifted(padded, comp, vec_neg(vec_add(plus_first, plus_second))))

    laplace = []
    elastic = []
    for comp in range(3):
        lap_comp = seconds[comp][0] + seconds[comp][1] + seconds[comp][2]
        grad_div = seconds[comp][comp]
        for other in range(3):
            if other != comp:
                grad_div = grad_div + mixed(other, comp, other)
        laplace.append(lap_comp)
        elastic.append((lame_first + shear) * grad_div + shear * lap_comp)
    return jnp.stack(elastic), jnp.stack(laplace)


def reference(field_now, field_before, lame_lambda, shear_modulus, density, source_field, wavelet, prior_mean, steps_taken, grad_change):
    coeff = 0.04 / density
    current = field_now
    earlier = field_before
    correlation = jnp.zeros(shear_modulus.shape, jnp.float32)
    for step in range(STEPS):
        extended = jnp.pad(current, ((0, 0), (1, 1), (0, 0), (0, 0)))
        elastic, laplace = operate(extended, lame_lambda, shear_modulus)
        correlation = correlation + jnp.sum(current * laplace, axis=0)
        nxt = 2.0 * current - earlier + coeff * (elastic + wavelet[step] * source_field)
        earlier = current
        current = nxt
    gradient = (shear_modulus - prior_mean) + 0.02 * correlation
    curv = [jnp.sum(steps_taken[i] * grad_change[i]) for i in range(PAIRS)]
    query = gradient
    alphas = [None] * PAIRS
    for i in reversed(range(PAIRS)):
        alphas[i] = jnp.sum(steps_taken[i] * query) / curv[i]
        query = query - alphas[i] * grad_change[i]
    newest = grad_change[PAIRS - 1]
    result = (curv[PAIRS - 1] / jnp.sum(newest * newest)) * query
    for i in range(PAIRS):
        beta = jnp.sum(grad_change[i] * result) / curv[i]
        result = result + (alphas[i] - beta) * steps_taken[i]
    return current, gradient, -result
```

```python
import functools

import jax
import jax.numpy as jnp
from jax import lax
from jax.experimental import pallas as pl
from jax.experimental.pallas import tpu as pltpu
from jax.sharding import PartitionSpec as P

PAD = 8
CHUNK_ROWS = 32
PIECES = 4


def chunk_rows(rows):
    size = CHUNK_ROWS
    while rows % size:
        size //= 2
    return size


def tile(start):
    return pl.ds(pl.multiple_of(start, 8), 8)


def fold(value):
    out = value[:, 0:128]
    for k in range(1, value.shape[1] // 128):
        out = out + value[:, 128 * k : 128 * (k + 1)]
    return out


def whole(value):
    return jnp.sum(jnp.sum(value, axis=0, keepdims=True), axis=1, keepdims=True)


def product_pairs(pairs):
    found = [(i, pairs + j) for i in range(pairs) for j in range(pairs)]
    return found + [(pairs + i, pairs + j) for i in range(pairs) for j in range(i, pairs)]


def kernel(
    n,
    steps,
    pairs,
    size,
    now_hbm,
    before_hbm,
    lame_hbm,
    shear_hbm,
    density_hbm,
    source_hbm,
    wavelet_hbm,
    prior_hbm,
    taken_hbm,
    change_hbm,
    final,
    grad,
    taken,
    change,
    summed,
    even,
    odd,
    lame,
    shear,
    coeff,
    source,
    prior,
    wavelet,
    sums,
    part,
    gathered,
    load_sem,
    send_sem,
    recv_sem,
    part_sem,
):
    me = lax.axis_index("gz")
    rows, cols = lame.shape[1], lame.shape[2]
    chunks = rows // size
    tiles = size // 8
    has_low = me > 0
    has_high = me < n - 1
    inside = pl.ds(PAD, rows)
    chained = n - 1 <= steps

    barrier = pltpu.get_barrier_semaphore()

    def greet(device):
        pl.semaphore_signal(
            barrier, inc=1, device_id={"gz": device}, device_id_type=pl.DeviceIdType.MESH
        )

    if chained:

        @pl.when(has_low)
        def _():
            greet(me - 1)

        @pl.when(has_high)
        def _():
            greet(me + 1)

    else:
        for k in range(1, n):
            greet(lax.rem(me + k, n))

    loads = [
        pltpu.make_async_copy(src, dst, load_sem.at[i])
        for i, src, dst in (
            (
                0,
                now_hbm.at[:, :, pl.ds(0, size)],
                even.at[:, pl.ds(1, 2), pl.ds(PAD, size)],
            ),
            (
                1,
                now_hbm.at[:, :, pl.ds(size, rows - size)],
                even.at[:, pl.ds(1, 2), pl.ds(PAD + size, rows - size)],
            ),
            (2, lame_hbm, lame),
            (3, shear_hbm, shear),
            (4, density_hbm, coeff),
            (5, before_hbm, odd.at[:, pl.ds(1, 2), inside]),
            (6, source_hbm, source),
            (7, wavelet_hbm, wavelet),
            (8, taken_hbm, taken),
            (9, change_hbm, change),
            (10, prior_hbm, prior),
        )
    ]
    for load in loads:
        load.start()

    def rdma(ref, parity, up, where, sem):
        side = 0 if up else 1
        target = lax.rem(me + (1 if up else n - 1), n)
        return pltpu.make_async_remote_copy(
            src_ref=ref.at[:, 2 if up else 1, where],
            dst_ref=ref.at[:, 0 if up else 3, where],
            send_sem=send_sem.at[parity, side],
            recv_sem=sem,
            device_id={"gz": target},
            device_id_type=pl.DeviceIdType.MESH,
        )

    def halo(ref, parity, up, chunk):
        where = pl.ds(pl.multiple_of(PAD + chunk * size, 8), size)
        return rdma(ref, parity, up, where, recv_sem.at[parity, 0 if up else 1, chunk])

    def send(ref, parity, chunk):
        @pl.when(has_high)
        def _():
            halo(ref, parity, True, chunk).start()

        @pl.when(has_low)
        def _():
            halo(ref, parity, False, chunk).start()

    def sent(ref, parity):
        @pl.when(has_high)
        def _():
            rdma(ref, parity, True, inside, recv_sem.at[parity, 0, 0]).wait_send()

        @pl.when(has_low)
        def _():
            rdma(ref, parity, False, inside, recv_sem.at[parity, 1, 0]).wait_send()

    def received(ref, parity, chunk):
        @pl.when(has_low)
        def _():
            halo(ref, parity, True, chunk).wait_recv()

        @pl.when(has_high)
        def _():
            halo(ref, parity, False, chunk).wait_recv()

    loads[0].wait()
    if chained:
        pl.semaphore_wait(barrier, has_low.astype(jnp.int32) + has_high.astype(jnp.int32))
    else:
        pl.semaphore_wait(barrier, n - 1)

    send(even, 0, 0)
    loads[1].wait()

    def first(chunk, carry):
        send(even, 0, chunk)
        return carry

    lax.fori_loop(1, chunks, first, 0)

    edge = jnp.zeros((even.shape[0], 4, PAD, cols), jnp.float32)
    for ref in (even, odd):
        ref[:, :, pl.ds(0, PAD)] = edge
        ref[:, :, pl.ds(PAD + rows, PAD)] = edge

    def clear(plane):
        def body(t, carry):
            for ref in (even, odd):
                for comp in range(3):
                    ref[comp, plane, tile(PAD + 8 * t)] = jnp.zeros((8, cols), jnp.float32)
            return carry

        lax.fori_loop(0, rows // 8, body, 0)

    @pl.when(me == 0)
    def _():
        clear(0)

    @pl.when(me == n - 1)
    def _():
        clear(3)

    for load in loads[2:5]:
        load.wait()

    def prepare(t, carry):
        for plane in range(2):
            at = (plane, tile(8 * t))
            lame[at] = lame[at] + shear[at]
            coeff[at] = 0.04 / coeff[at]
            grad[at] = jnp.zeros((8, cols), jnp.float32)
        return carry

    lax.fori_loop(0, rows // 8, prepare, 0)
    for load in loads[5:]:
        load.wait()

    products = product_pairs(pairs)
    count = len(products)

    def stored(t, totals):
        totals = list(totals)
        for plane in range(2):
            vectors = [taken[i, plane, tile(8 * t)] for i in range(pairs)]
            vectors += [change[i, plane, tile(8 * t)] for i in range(pairs)]
            for k, (a, b) in enumerate(products):
                totals[k] = totals[k] + fold(vectors[a] * vectors[b])
        return tuple(totals)

    totals = lax.fori_loop(
        0, rows // 8, stored, tuple(jnp.zeros((8, 128), jnp.float32) for _ in products)
    )
    place = lax.broadcasted_iota(jnp.int32, (1, 128), 1)

    line = jnp.zeros((1, 128), jnp.float32)
    for k in range(count):
        line = jnp.where(place == k, whole(totals[k]), line)
    part[...] = line
    for i in range(2 * pairs):
        sums[i] = jnp.zeros((8, 128), jnp.float32)

    row_at = lax.broadcasted_iota(jnp.int32, (8, cols), 0)
    col_at = lax.broadcasted_iota(jnp.int32, (8, cols), 1)
    is_top, is_bottom = row_at == 0, row_at == 7
    is_left, is_right = col_at == 0, col_at == cols - 1

    def along_x(previous, value, following):
        minus = pltpu.roll(jnp.where(is_bottom, previous, value), 1, 0)
        plus = pltpu.roll(jnp.where(is_top, following, value), 7, 0)
        return minus, plus

    def along_y(value):
        minus = jnp.where(is_left, 0.0, pltpu.roll(value, 1, 1))
        plus = jnp.where(is_right, 0.0, pltpu.roll(value, cols - 1, 1))
        return minus, plus

    def delta_y(value):
        minus, plus = along_y(value)
        return plus - minus

    def correlate(current, t):
        def load(comp, plane, shift=0):
            return current[comp, plane, tile(PAD + 8 * (t + shift))]

        values = []
        for plane in range(2):
            low, mid, high = plane, plane + 1, plane + 2
            value = None
            for comp in range(3):
                centre = load(comp, mid)
                minus_x, plus_x = along_x(load(comp, mid, -1), centre, load(comp, mid, 1))
                minus_y, plus_y = along_y(centre)
                lap = (
                    (load(comp, high) + load(comp, low)) + (minus_x + plus_x)
                ) + ((minus_y + plus_y) - 6.0 * centre)
                value = centre * lap if value is None else value + centre * lap
            values.append(value)
        return values

    def update(step, current, other, t, last=False):
        amplitude = wavelet[step]

        def load(comp, plane, shift=0):
            return current[comp, plane, tile(PAD + 8 * (t + shift))]

        for plane in range(2):
            low, mid, high = plane, plane + 1, plane + 2
            at = tile(8 * t)
            here = tile(PAD + 8 * t)

            def delta_z(comp, shift=0):
                return load(comp, high, shift) - load(comp, low, shift)

            def delta_xz(comp, centre):
                minus, plus = along_x(delta_z(comp, -1), centre, delta_z(comp, 1))
                return plus - minus

            centre = [load(comp, mid) for comp in range(3)]
            diff = [delta_z(comp) for comp in range(3)]
            total = [load(comp, high) + load(comp, low) for comp in range(3)]
            xs = [along_x(load(comp, mid, -1), centre[comp], load(comp, mid, 1)) for comp in range(3)]
            ys = [along_y(centre[comp]) for comp in range(3)]
            sum_x = [minus + plus for minus, plus in xs]
            sum_y = [minus + plus for minus, plus in ys]
            dx = [plus - minus for minus, plus in xs]
            lap = [
                (total[comp] + sum_x[comp]) + (sum_y[comp] - 6.0 * centre[comp])
                for comp in range(3)
            ]
            mixed = [
                delta_xz(1, diff[1]) + delta_y(diff[2]),
                delta_xz(0, diff[0]) + delta_y(dx[2]),
                delta_y(diff[0] + dx[1]),
            ]
            own = [total[0], sum_x[1], sum_y[2]]
            both = lame[plane, at]
            mu = shear[plane, at]
            rate = coeff[plane, at]
            if not last:
                grad[plane, at] = grad[plane, at] + (
                    centre[0] * lap[0] + centre[1] * lap[1] + centre[2] * lap[2]
                )
            for comp in range(3):
                doubled = 2.0 * centre[comp]
                elastic = both * ((own[comp] - doubled) + 0.25 * mixed[comp]) + mu * lap[comp]
                value = (
                    doubled
                    - other[comp, mid, here]
                    + rate * (elastic + amplitude * source[comp, plane, at])
                )
                if last:
                    final[comp, plane, at] = value
                else:
                    other[comp, mid, here] = value

    def finish(current, t, totals):
        totals = list(totals)
        newest = correlate(current, t)
        for plane in range(2):
            at = (plane, tile(8 * t))
            value = (shear[at] - prior[at]) + 0.02 * (grad[at] + newest[plane])
            grad[at] = value
            for i in range(pairs):
                totals[i] = totals[i] + fold(taken[(i,) + at] * value)
                totals[pairs + i] = totals[pairs + i] + fold(change[(i,) + at] * value)
        return tuple(totals)

    def over_tiles(chunk, body):
        def tile_body(t, carry):
            body(chunk * tiles + t)
            return carry

        lax.fori_loop(0, tiles, tile_body, 0)

    def advance(step, current, other, parity):
        @pl.when(step > 0)
        def _():
            sent(other, 1 - parity)

        received(current, parity, 0)

        def chunk_body(chunk, carry):
            @pl.when(chunk + 1 < chunks)
            def _():
                received(current, parity, chunk + 1)

            over_tiles(chunk, lambda t: update(step, current, other, t))
            send(other, 1 - parity, chunk)
            return carry

        lax.fori_loop(0, chunks, chunk_body, 0)

    def two_steps(k, carry):
        advance(2 * k, even, odd, 0)
        advance(2 * k + 1, odd, even, 1)
        return carry

    lax.fori_loop(0, steps // 2 - 1, two_steps, 0)
    advance(steps - 2, even, odd, 0)

    def last_body(chunk, carry):
        received(odd, 1, chunk)
        totals = lax.fori_loop(
            chunk * tiles,
            chunk * tiles + tiles,
            functools.partial(finish, odd),
            tuple(sums[i] for i in range(2 * pairs)),
        )
        for i in range(2 * pairs):
            sums[i] = totals[i]

        @pl.when((chunk > 0) & (chunk < chunks - 1))
        def _():
            over_tiles(chunk - 1, lambda t: update(steps - 1, odd, even, t, True))

        return carry

    lax.fori_loop(0, chunks, last_body, 0)

    line = part[...]
    for i in range(2 * pairs):
        line = jnp.where(place == count + i, whole(sums[i]), line)
    part[...] = line

    def exchange(src, dst, target):
        return pltpu.make_async_remote_copy(
            src_ref=src,
            dst_ref=dst,
            send_sem=part_sem.at[0],
            recv_sem=part_sem.at[1],
            device_id={"gz": target},
            device_id_type=pl.DeviceIdType.MESH,
        )

    for k in range(1, n):
        exchange(part, gathered.at[k - 1], lax.rem(me + k, n)).start()

    for chunk in range(max(chunks - 2, 0), chunks):
        over_tiles(chunk, lambda t: update(steps - 1, odd, even, t, True))

    sent(even, 0)
    sent(odd, 1)
    everything = exchange(gathered, gathered, lax.rem(me + 1, n))
    everything.wait_recv()
    line = part[...]
    for k in range(n - 1):
        line = line + gathered[k]
    summed[...] = line
    everything.wait_send()


def publish(
    pairs,
    final,
    grad,
    taken,
    change,
    summed,
    final_hbm,
    grad_hbm,
    direction_hbm,
    direction,
    sem,
):
    rows, cols = grad.shape[1], grad.shape[2]
    copies = [
        pltpu.make_async_copy(final, final_hbm, sem.at[0]),
        pltpu.make_async_copy(grad, grad_hbm, sem.at[1]),
    ]
    for copy in copies:
        copy.start()

    place = lax.broadcasted_iota(jnp.int32, (1, 128), 1)
    products = product_pairs(pairs)
    count = len(products)
    where_of = {pair: k for k, pair in enumerate(products)}
    for i in range(2 * pairs):
        where_of[(i, 2 * pairs)] = count + i
    line = summed[...]
    cache = {}

    def inner(a, b):
        key = (min(a, b), max(a, b))
        if key not in cache:
            chosen = jnp.where(place == where_of[key], line, 0.0)
            cache[key] = jnp.sum(chosen, axis=1, keepdims=True)
        return cache[key]

    gradient_at = 2 * pairs
    curvature = [inner(i, pairs + i) for i in range(pairs)]
    alphas = [None] * pairs
    for i in reversed(range(pairs)):
        value = inner(i, gradient_at)
        for j in range(i + 1, pairs):
            value = value - alphas[j] * inner(i, pairs + j)
        alphas[i] = value / curvature[i]
    newest = 2 * pairs - 1
    gamma = curvature[pairs - 1] / inner(newest, newest)
    changes = [-gamma * alphas[i] for i in range(pairs)]
    steps_coef = [None] * pairs
    for i in range(pairs):
        value = gamma * inner(pairs + i, gradient_at)
        for j in range(pairs):
            value = value + changes[j] * inner(pairs + i, pairs + j)
        for j in range(i):
            value = value + steps_coef[j] * inner(j, pairs + i)
        steps_coef[i] = alphas[i] - value / curvature[i]

    def spread(value):
        return -jnp.broadcast_to(value, (8, cols))

    by_grad = spread(gamma)
    by_taken = [spread(value) for value in steps_coef]
    by_change = [spread(value) for value in changes]

    def combine(t, carry):
        for plane in range(2):
            at = (plane, tile(8 * t))
            value = by_grad * grad[at]
            for i in range(pairs):
                value = value + by_taken[i] * taken[(i,) + at]
                value = value + by_change[i] * change[(i,) + at]
            direction[at] = value
        return carry

    tiles = rows // 8
    pieces = PIECES
    while tiles % pieces:
        pieces -= 1
    for piece in range(pieces):
        first, count = piece * (tiles // pieces), tiles // pieces
        lax.fori_loop(first, first + count, combine, 0)
        span = pl.ds(8 * first, 8 * count)
        copy = pltpu.make_async_copy(
            direction.at[:, span], direction_hbm.at[:, span], sem.at[2 + piece]
        )
        copy.start()
        copies.append(copy)
    for copy in copies:
        copy.wait()


def on_device(
    n,
    field_now,
    field_before,
    lame_lambda,
    shear_modulus,
    density,
    source_field,
    wavelet,
    prior_mean,
    steps_taken,
    grad_change,
):
    comps, depth, rows, cols = field_now.shape
    pairs = steps_taken.shape[0]
    steps = wavelet.shape[0]
    size = chunk_rows(rows)
    chunks = rows // size
    f32 = jnp.float32
    state = pltpu.VMEM((comps, depth + 2, rows + 2 * PAD, cols), f32)
    model = pltpu.VMEM((depth, rows, cols), f32)
    dma = pltpu.SemaphoreType.DMA
    anywhere = pl.BlockSpec(memory_space=pltpu.HBM)
    free = pl.BlockSpec(memory_space=pl.ANY)
    in_vmem = pl.BlockSpec(memory_space=pltpu.VMEM)
    results = pl.pallas_call(
        functools.partial(kernel, n, steps, pairs, size),
        out_shape=(
            pltpu.VMEM(field_now.shape, f32),
            pltpu.VMEM(lame_lambda.shape, f32),
            pltpu.VMEM(steps_taken.shape, f32),
            pltpu.VMEM(grad_change.shape, f32),
            pltpu.VMEM((1, 128), f32),
        ),
        in_specs=[anywhere] * 10,
        out_specs=(in_vmem,) * 5,
        scratch_shapes=[
            state,
            state,
            model,
            model,
            model,
            pltpu.VMEM((comps, depth, rows, cols), f32),
            model,
            pltpu.SMEM((steps,), f32),
            pltpu.VMEM((2 * pairs, 8, 128), f32),
            pltpu.VMEM((1, 128), f32),
            pltpu.VMEM((n - 1, 1, 128), f32),
            dma((11,)),
            dma((2, 2)),
            dma((2, 2, chunks)),
            dma((2,)),
        ],
        compiler_params=pltpu.CompilerParams(
            collective_id=0, has_side_effects=True, vmem_limit_bytes=63000000
        ),
    )(
        field_now,
        field_before,
        lame_lambda,
        shear_modulus,
        density,
        source_field,
        wavelet,
        prior_mean,
        steps_taken,
        grad_change,
    )
    return pl.pallas_call(
        functools.partial(publish, pairs),
        out_shape=tuple(
            jax.ShapeDtypeStruct(shape, f32)
            for shape in (field_now.shape, lame_lambda.shape, lame_lambda.shape)
        ),
        in_specs=[in_vmem] * 5,
        out_specs=(free, free, free),
        scratch_shapes=[model, dma((2 + PIECES,))],
        compiler_params=pltpu.CompilerParams(vmem_limit_bytes=4 * 1024 * 1024),
    )(*[pltpu.with_memory_space_constraint(value, pltpu.VMEM) for value in results])


def solution(mesh):
    n = mesh.shape["gz"]
    fields = P("sample", "gz", None, None)
    models = P("gz", "sample", None)
    placed = (
        fields,
        fields,
        models,
        models,
        models,
        fields,
        P("sample"),
        models,
        fields,
        fields,
    )
    return jax.shard_map(
        functools.partial(on_device, n),
        mesh=mesh,
        in_specs=placed,
        out_specs=(fields, models, models),
        check_vma=False,
    )
```

```python
import functools

import jax
import jax.numpy as jnp
from jax import lax
from jax.experimental import pallas as pl
from jax.experimental.pallas import tpu as pltpu
from jax.sharding import PartitionSpec as P

PAD = 8
CHUNK_ROWS = 16
PIECES = 4


def chunk_rows(rows):
    size = CHUNK_ROWS
    while rows % size:
        size //= 2
    return size


def tile(start):
    return pl.ds(pl.multiple_of(start, 8), 8)


def fold(value):
    out = value[:, 0:128]
    for k in range(1, value.shape[1] // 128):
        out = out + value[:, 128 * k : 128 * (k + 1)]
    return out


def whole(value):
    return jnp.sum(jnp.sum(value, axis=0, keepdims=True), axis=1, keepdims=True)


def product_pairs(pairs):
    found = [(i, pairs + j) for i in range(pairs) for j in range(pairs)]
    return found + [(pairs + i, pairs + j) for i in range(pairs) for j in range(i, pairs)]


def kernel(
    n,
    steps,
    pairs,
    size,
    relayed,
    now_hbm,
    before_hbm,
    lame_hbm,
    shear_hbm,
    density_hbm,
    source_hbm,
    wavelet_hbm,
    prior_hbm,
    taken_hbm,
    change_hbm,
    final,
    grad,
    pool,
    summed,
    even,
    odd,
    models,
    source,
    wavelet,
    sums,
    part,
    gathered,
    product_out,
    product_in,
    load_sem,
    send_sem,
    inner_sem,
    outer_sem,
    product_sem,
    part_sem,
):
    me = lax.axis_index("gz")
    rows, cols = grad.shape[1], grad.shape[2]
    chunks = rows // size
    tiles = size // 8
    upper = lax.rem(me, 2)
    has_outer = (me > 0) & (me < n - 1)
    inside = pl.ds(PAD, rows)
    chained = n - 1 <= steps
    inner_target = me + 1 - 2 * upper
    outer_target = lax.rem(me + n - 1 + 2 * upper, n)
    inner_plane, outer_plane = 2 - upper, 1 + upper
    inner_halo, outer_halo = 3 - 3 * upper, 3 * upper
    early = relayed * upper
    late = relayed - early
    lame, shear, coeff, prior = (models.at[i] for i in range(4))
    taken, change = pool.at[pl.ds(0, pairs)], pool.at[pl.ds(pairs, pairs)]

    barrier = pltpu.get_barrier_semaphore()

    def greet(device):
        pl.semaphore_signal(
            barrier, inc=1, device_id={"gz": device}, device_id_type=pl.DeviceIdType.MESH
        )

    if chained:

        @pl.when(has_outer)
        def _():
            greet(outer_target)

        greet(inner_target)
    else:
        for k in range(1, n):
            greet(lax.rem(me + k, n))

    loads = [
        pltpu.make_async_copy(src, dst, load_sem.at[i])
        for i, src, dst in (
            (
                0,
                now_hbm.at[:, :, pl.ds(0, size)],
                even.at[:, pl.ds(1, 2), pl.ds(PAD, size)],
            ),
            (
                1,
                now_hbm.at[:, :, pl.ds(size, rows - size)],
                even.at[:, pl.ds(1, 2), pl.ds(PAD + size, rows - size)],
            ),
            (2, lame_hbm, lame),
            (2, shear_hbm, shear),
            (2, density_hbm, coeff),
            (2, prior_hbm, prior),
            (3, before_hbm, odd.at[:, pl.ds(1, 2), inside]),
            (4, source_hbm, source),
            (5, wavelet_hbm, wavelet),
            (6, taken_hbm, taken),
            (6, change_hbm, change),
        )
    ]
    for load in loads:
        load.start()

    def remote(src, dst, send, recv, target):
        return pltpu.make_async_remote_copy(
            src_ref=src,
            dst_ref=dst,
            send_sem=send,
            recv_sem=recv,
            device_id={"gz": target},
            device_id_type=pl.DeviceIdType.MESH,
        )

    def span(chunk):
        return pl.ds(pl.multiple_of(PAD + chunk * size, 8), size)

    def send_inner(ref, parity, chunk):
        remote(
            ref.at[:, inner_plane, span(chunk)],
            ref.at[:, 3 * upper, span(chunk)],
            send_sem.at[parity],
            inner_sem.at[parity],
            inner_target,
        ).start()

    def send_outer(ref, parity, chunk):
        remote(
            ref.at[:, outer_plane, span(chunk)],
            ref.at[:, 3 - 3 * upper, span(chunk)],
            send_sem.at[parity],
            outer_sem.at[parity, chunk],
            outer_target,
        ).start()

    def send(ref, parity, chunk):
        @pl.when(has_outer)
        def _():
            send_outer(ref, parity, chunk)

        send_inner(ref, parity, chunk)

    def sent(ref, parity):
        def wait(planes):
            whole_planes = ref.at[:, planes, inside]
            remote(
                whole_planes, whole_planes, send_sem.at[parity], inner_sem.at[parity], inner_target
            ).wait_send()

        @pl.when(has_outer)
        def _():
            wait(pl.ds(1, 2))

        @pl.when(jnp.logical_not(has_outer))
        def _():
            wait(pl.ds(1, 1))

    def received_inner(ref, parity):
        halo = ref.at[:, inner_halo, inside]
        remote(halo, halo, send_sem.at[parity], inner_sem.at[parity], inner_target).wait_recv()

    def received_outer(ref, parity, chunk):
        halo = ref.at[:, outer_halo, span(chunk)]
        remote(
            halo, halo, send_sem.at[parity], outer_sem.at[parity, chunk], outer_target
        ).wait_recv()

    loads[0].wait()
    if chained:
        pl.semaphore_wait(barrier, 1 + has_outer.astype(jnp.int32))
    else:
        pl.semaphore_wait(barrier, n - 1)

    send(even, 0, 0)
    loads[1].wait()

    def first(chunk, carry):
        send(even, 0, chunk)
        return carry

    lax.fori_loop(1, chunks, first, 0)

    edge = jnp.zeros((even.shape[0], 4, PAD, cols), jnp.float32)
    for ref in (even, odd):
        ref[:, :, pl.ds(0, PAD)] = edge
        ref[:, :, pl.ds(PAD + rows, PAD)] = edge

    @pl.when(jnp.logical_not(has_outer))
    def _():
        def body(t, carry):
            for ref in (even, odd):
                for comp in range(3):
                    ref[comp, outer_halo, tile(PAD + 8 * t)] = jnp.zeros((8, cols), jnp.float32)
            return carry

        lax.fori_loop(0, rows // 8, body, 0)

    pltpu.make_async_copy(models, models, load_sem.at[2]).wait()

    def prepare(t, carry):
        for plane in range(2):
            at = (plane, tile(8 * t))
            lame[at] = lame[at] + shear[at]
            coeff[at] = 0.04 / coeff[at]
            grad[at] = jnp.zeros((8, cols), jnp.float32)
        return carry

    lax.fori_loop(0, rows // 8, prepare, 0)
    for load in loads[6:9]:
        load.wait()
    pltpu.make_async_copy(pool, pool, load_sem.at[6]).wait()

    products = product_pairs(pairs)
    count = len(products)

    def stored(t, totals):
        totals = list(totals)
        for plane in range(2):
            vectors = [pool[i, plane, tile(8 * t)] for i in range(2 * pairs)]
            for k, (a, b) in enumerate(products):
                totals[k] = totals[k] + fold(vectors[a] * vectors[b])
        return tuple(totals)

    totals = lax.fori_loop(
        0, rows // 8, stored, tuple(jnp.zeros((8, 128), jnp.float32) for _ in products)
    )
    place = lax.broadcasted_iota(jnp.int32, (1, 128), 1)

    line = jnp.zeros((1, 128), jnp.float32)
    for k in range(count):
        line = jnp.where(place == k, whole(totals[k]), line)
    part[...] = line

    row_at = lax.broadcasted_iota(jnp.int32, (8, cols), 0)
    col_at = lax.broadcasted_iota(jnp.int32, (8, cols), 1)
    is_top, is_bottom = row_at == 0, row_at == 7
    is_left, is_right = col_at == 0, col_at == cols - 1

    def along_x(previous, value, following):
        minus = pltpu.roll(jnp.where(is_bottom, previous, value), 1, 0)
        plus = pltpu.roll(jnp.where(is_top, following, value), 7, 0)
        return minus, plus

    def along_y(value):
        minus = jnp.where(is_left, 0.0, pltpu.roll(value, 1, 1))
        plus = jnp.where(is_right, 0.0, pltpu.roll(value, cols - 1, 1))
        return minus, plus

    def delta_y(value):
        minus, plus = along_y(value)
        return plus - minus

    def update(step, current, other, t, last=False):
        amplitude = wavelet[step]

        def load(comp, plane, shift=0):
            return current[comp, plane, tile(PAD + 8 * (t + shift))]

        for plane in range(2):
            low, mid, high = plane, plane + 1, plane + 2
            at = tile(8 * t)
            here = tile(PAD + 8 * t)

            def delta_z(comp, shift=0):
                return load(comp, high, shift) - load(comp, low, shift)

            def delta_xz(comp, centre):
                minus, plus = along_x(delta_z(comp, -1), centre, delta_z(comp, 1))
                return plus - minus

            centre = [load(comp, mid) for comp in range(3)]
            diff = [delta_z(comp) for comp in range(3)]
            total = [load(comp, high) + load(comp, low) for comp in range(3)]
            xs = [along_x(load(comp, mid, -1), centre[comp], load(comp, mid, 1)) for comp in range(3)]
            ys = [along_y(centre[comp]) for comp in range(3)]
            sum_x = [minus + plus for minus, plus in xs]
            sum_y = [minus + plus for minus, plus in ys]
            dx = [plus - minus for minus, plus in xs]
            lap = [
                (total[comp] + sum_x[comp]) + (sum_y[comp] - 6.0 * centre[comp])
                for comp in range(3)
            ]
            mixed = [
                delta_xz(1, diff[1]) + delta_y(diff[2]),
                delta_xz(0, diff[0]) + delta_y(dx[2]),
                delta_y(diff[0] + dx[1]),
            ]
            own = [total[0], sum_x[1], sum_y[2]]
            both = lame[plane, at]
            mu = shear[plane, at]
            rate = coeff[plane, at]
            if not last:
                grad[plane, at] = grad[plane, at] + (
                    centre[0] * lap[0] + centre[1] * lap[1] + centre[2] * lap[2]
                )
            for comp in range(3):
                doubled = 2.0 * centre[comp]
                elastic = both * ((own[comp] - doubled) + 0.25 * mixed[comp]) + mu * lap[comp]
                value = (
                    doubled
                    - other[comp, mid, here]
                    + rate * (elastic + amplitude * source[comp, plane, at])
                )
                if last:
                    final[comp, plane, at] = value
                else:
                    other[comp, mid, here] = value

    def over_tiles(chunk, body):
        def tile_body(t, carry):
            body(chunk * tiles + t)
            return carry

        lax.fori_loop(0, tiles, tile_body, 0)

    def wait_outer(ref, parity, chunk):
        @pl.when(has_outer)
        def _():
            received_outer(ref, parity, chunk)

    def advance(step, current, other, parity, relay):
        @pl.when(step > 0)
        def _():
            sent(other, 1 - parity)

        received_inner(current, parity)
        wait_outer(current, parity, 0)

        def chunk_body(chunk, carry):
            @pl.when(chunk + 1 < chunks)
            def _():
                wait_outer(current, parity, chunk + 1)

            over_tiles(chunk, lambda t: update(step, current, other, t))
            if relay:

                @pl.when(has_outer & ((chunk < early) | (chunk >= early + relayed)))
                def _():
                    send_outer(other, 1 - parity, chunk)

                send_inner(other, 1 - parity, chunk)
            else:
                send(other, 1 - parity, chunk)
            return carry

        lax.fori_loop(0, chunks, chunk_body, 0)

    def two_steps(k, carry):
        advance(2 * k, even, odd, 0, False)
        advance(2 * k + 1, odd, even, 1, False)
        return carry

    lax.fori_loop(0, steps // 2 - 1, two_steps, 0)
    advance(steps - 2, even, odd, 0, True)

    def across(t):
        here = tile(PAD + 8 * t)
        value = odd[0, outer_plane, here] * odd[0, outer_halo, here]
        for comp in range(1, 3):
            value = value + odd[comp, outer_plane, here] * odd[comp, outer_halo, here]
        return value

    returned = remote(
        product_out, product_in, product_sem.at[0], product_sem.at[1], outer_target
    )
    if relayed:

        @pl.when(has_outer)
        def _():
            def multiply(chunk, carry):
                received_outer(odd, 1, early + chunk)

                def body(t, inner):
                    product_out[tile(8 * t)] = across(early * tiles + t)
                    return inner

                lax.fori_loop(chunk * tiles, chunk * tiles + tiles, body, 0)
                return carry

            lax.fori_loop(0, relayed, multiply, 0)
            returned.start()

            def follow(chunk, carry):
                send_outer(odd, 1, early + chunk)
                return carry

            lax.fori_loop(0, relayed, follow, 0)

    received_inner(odd, 1)

    def weigh(totals, at, value):
        return tuple(
            totals[i] + fold(pool[(i,) + at] * value) for i in range(2 * pairs)
        )

    def own_part(t, totals):
        def load(comp, plane, shift=0):
            return odd[comp, plane, tile(PAD + 8 * (t + shift))]

        for mid, around in ((inner_plane, (outer_plane, inner_halo)), (outer_plane, (inner_plane,))):
            at = (mid - 1, tile(8 * t))
            value = None
            for comp in range(3):
                centre = load(comp, mid)
                minus_x, plus_x = along_x(load(comp, mid, -1), centre, load(comp, mid, 1))
                minus_y, plus_y = along_y(centre)
                total = load(comp, around[0])
                for plane in around[1:]:
                    total = total + load(comp, plane)
                lap = (total + (minus_x + plus_x)) + ((minus_y + plus_y) - 6.0 * centre)
                value = centre * lap if value is None else value + centre * lap
            value = (shear[at] - prior[at]) + 0.02 * (grad[at] + value)
            grad[at] = value
            totals = weigh(totals, at, value)
        return totals

    totals = lax.fori_loop(
        0,
        rows // 8,
        own_part,
        tuple(jnp.zeros((8, 128), jnp.float32) for _ in range(2 * pairs)),
    )
    for i in range(2 * pairs):
        sums[i] = totals[i]

    @pl.when(has_outer)
    def _():
        def add(product):
            def body(t, totals):
                at = (outer_plane - 1, tile(8 * t))
                value = 0.02 * product(t)
                grad[at] = grad[at] + value
                return weigh(totals, at, value)

            return body

        totals = tuple(sums[i] for i in range(2 * pairs))
        if relayed:
            totals = lax.fori_loop(
                early * tiles,
                (early + relayed) * tiles,
                add(lambda t: product_out[tile(8 * (t - early * tiles))]),
                totals,
            )

        def direct(chunk, totals):
            received_outer(odd, 1, chunk)
            return lax.fori_loop(chunk * tiles, chunk * tiles + tiles, add(across), totals)

        totals = lax.fori_loop(2 * relayed, chunks, direct, totals)
        if relayed:
            returned.wait_recv()
            totals = lax.fori_loop(
                late * tiles,
                (late + relayed) * tiles,
                add(lambda t: product_in[tile(8 * (t - late * tiles))]),
                totals,
            )
        for i in range(2 * pairs):
            sums[i] = totals[i]

    line = part[...]
    for i in range(2 * pairs):
        line = jnp.where(place == count + i, whole(sums[i]), line)
    part[...] = line

    def exchange(src, dst, target):
        return remote(src, dst, part_sem.at[0], part_sem.at[1], target)

    for k in range(1, n):
        exchange(part, gathered.at[k - 1], lax.rem(me + k, n)).start()

    def close(chunk, carry):
        over_tiles(chunk, lambda t: update(steps - 1, odd, even, t, True))
        return carry

    ready = min(2 * relayed + 1, chunks) if relayed else 0
    lax.fori_loop(ready, chunks, close, 0)
    if relayed:

        @pl.when(has_outer)
        def _():
            def arrive(chunk, carry):
                received_outer(odd, 1, late + chunk)
                return carry

            lax.fori_loop(0, relayed, arrive, 0)

        lax.fori_loop(0, ready, close, 0)

        @pl.when(has_outer)
        def _():
            returned.wait_send()

    sent(even, 0)
    sent(odd, 1)
    everything = exchange(gathered, gathered, inner_target)
    everything.wait_recv()
    line = part[...]
    for k in range(n - 1):
        line = line + gathered[k]
    summed[...] = line
    everything.wait_send()


def publish(
    pairs,
    final,
    grad,
    pool,
    summed,
    final_hbm,
    grad_hbm,
    direction_hbm,
    direction,
    sem,
):
    rows, cols = grad.shape[1], grad.shape[2]
    copies = [
        pltpu.make_async_copy(final, final_hbm, sem.at[0]),
        pltpu.make_async_copy(grad, grad_hbm, sem.at[1]),
    ]
    for copy in copies:
        copy.start()

    place = lax.broadcasted_iota(jnp.int32, (1, 128), 1)
    products = product_pairs(pairs)
    count = len(products)
    where_of = {pair: k for k, pair in enumerate(products)}
    for i in range(2 * pairs):
        where_of[(i, 2 * pairs)] = count + i
    line = summed[...]
    cache = {}

    def inner(a, b):
        key = (min(a, b), max(a, b))
        if key not in cache:
            chosen = jnp.where(place == where_of[key], line, 0.0)
            cache[key] = jnp.sum(chosen, axis=1, keepdims=True)
        return cache[key]

    gradient_at = 2 * pairs
    curvature = [inner(i, pairs + i) for i in range(pairs)]
    alphas = [None] * pairs
    for i in reversed(range(pairs)):
        value = inner(i, gradient_at)
        for j in range(i + 1, pairs):
            value = value - alphas[j] * inner(i, pairs + j)
        alphas[i] = value / curvature[i]
    newest = 2 * pairs - 1
    gamma = curvature[pairs - 1] / inner(newest, newest)
    changes = [-gamma * alphas[i] for i in range(pairs)]
    steps_coef = [None] * pairs
    for i in range(pairs):
        value = gamma * inner(pairs + i, gradient_at)
        for j in range(pairs):
            value = value + changes[j] * inner(pairs + i, pairs + j)
        for j in range(i):
            value = value + steps_coef[j] * inner(j, pairs + i)
        steps_coef[i] = alphas[i] - value / curvature[i]

    def spread(value):
        return -jnp.broadcast_to(value, (8, cols))

    by_grad = spread(gamma)
    by_taken = [spread(value) for value in steps_coef]
    by_change = [spread(value) for value in changes]

    def combine(t, carry):
        for plane in range(2):
            at = (plane, tile(8 * t))
            value = by_grad * grad[at]
            for i in range(pairs):
                value = value + by_taken[i] * pool[(i,) + at]
                value = value + by_change[i] * pool[(pairs + i,) + at]
            direction[at] = value
        return carry

    tiles = rows // 8
    pieces = PIECES
    while tiles % pieces:
        pieces -= 1
    for piece in range(pieces):
        first, count = piece * (tiles // pieces), tiles // pieces
        lax.fori_loop(first, first + count, combine, 0, unroll=True)
        span = pl.ds(8 * first, 8 * count)
        copy = pltpu.make_async_copy(
            direction.at[:, span], direction_hbm.at[:, span], sem.at[2 + piece]
        )
        copy.start()
        copies.append(copy)
    for copy in copies:
        copy.wait()


def on_device(
    n,
    field_now,
    field_before,
    lame_lambda,
    shear_modulus,
    density,
    source_field,
    wavelet,
    prior_mean,
    steps_taken,
    grad_change,
):
    comps, depth, rows, cols = field_now.shape
    pairs = steps_taken.shape[0]
    steps = wavelet.shape[0]
    size = chunk_rows(rows)
    chunks = rows // size
    relayed = 3 * chunks // 10
    f32 = jnp.float32
    state = pltpu.VMEM((comps, depth + 2, rows + 2 * PAD, cols), f32)
    model = pltpu.VMEM((depth, rows, cols), f32)
    returned = pltpu.VMEM((max(relayed, 1) * size, cols), f32)
    dma = pltpu.SemaphoreType.DMA
    anywhere = pl.BlockSpec(memory_space=pltpu.HBM)
    free = pl.BlockSpec(memory_space=pl.ANY)
    in_vmem = pl.BlockSpec(memory_space=pltpu.VMEM)
    results = pl.pallas_call(
        functools.partial(kernel, n, steps, pairs, size, relayed),
        out_shape=(
            pltpu.VMEM(field_now.shape, f32),
            pltpu.VMEM(lame_lambda.shape, f32),
            pltpu.VMEM((2 * pairs,) + lame_lambda.shape, f32),
            pltpu.VMEM((1, 128), f32),
        ),
        in_specs=[anywhere] * 10,
        out_specs=(in_vmem,) * 4,
        scratch_shapes=[
            state,
            state,
            pltpu.VMEM((4, depth, rows, cols), f32),
            pltpu.VMEM((comps, depth, rows, cols), f32),
            pltpu.SMEM((steps,), f32),
            pltpu.VMEM((2 * pairs, 8, 128), f32),
            pltpu.VMEM((1, 128), f32),
            pltpu.VMEM((n - 1, 1, 128), f32),
            returned,
            returned,
            dma((7,)),
            dma((2,)),
            dma((2,)),
            dma((2, chunks)),
            dma((2,)),
            dma((2,)),
        ],
        compiler_params=pltpu.CompilerParams(
            collective_id=0, has_side_effects=True, vmem_limit_bytes=63000000
        ),
    )(
        field_now,
        field_before,
        lame_lambda,
        shear_modulus,
        density,
        source_field,
        wavelet,
        prior_mean,
        steps_taken,
        grad_change,
    )
    return pl.pallas_call(
        functools.partial(publish, pairs),
        out_shape=tuple(
            jax.ShapeDtypeStruct(shape, f32)
            for shape in (field_now.shape, lame_lambda.shape, lame_lambda.shape)
        ),
        in_specs=[in_vmem] * 4,
        out_specs=(free, free, free),
        scratch_shapes=[model, dma((2 + PIECES,))],
        compiler_params=pltpu.CompilerParams(vmem_limit_bytes=4 * 1024 * 1024),
    )(*[pltpu.with_memory_space_constraint(value, pltpu.VMEM) for value in results])


def solution(mesh):
    n = mesh.shape["gz"]
    fields = P("sample", "gz", None, None)
    models = P("gz", "sample", None)
    placed = (
        fields,
        fields,
        models,
        models,
        models,
        fields,
        P("sample"),
        models,
        fields,
        fields,
    )
    return jax.shard_map(
        functools.partial(on_device, n),
        mesh=mesh,
        in_specs=placed,
        out_specs=(fields, models, models),
        check_vma=False,
    )
```

```python
import functools

import jax
import jax.numpy as jnp
from jax import lax
from jax.experimental import pallas as pl
from jax.experimental.pallas import tpu as pltpu
from jax.sharding import PartitionSpec as P

PAD = 8
CHUNK_ROWS = 16
PIECES = 4


def chunk_rows(rows):
    size = CHUNK_ROWS
    while rows % size:
        size //= 2
    return size


def tile(start):
    return pl.ds(pl.multiple_of(start, 8), 8)


def fold(value):
    out = value[:, 0:128]
    for k in range(1, value.shape[1] // 128):
        out = out + value[:, 128 * k : 128 * (k + 1)]
    return out


def whole(value):
    return jnp.sum(jnp.sum(value, axis=0, keepdims=True), axis=1, keepdims=True)


def product_pairs(pairs):
    found = [(i, pairs + j) for i in range(pairs) for j in range(pairs)]
    return found + [(pairs + i, pairs + j) for i in range(pairs) for j in range(i, pairs)]


def kernel(
    n,
    steps,
    pairs,
    size,
    relayed,
    now_hbm,
    before_hbm,
    lame_hbm,
    shear_hbm,
    density_hbm,
    source_hbm,
    wavelet_hbm,
    prior_hbm,
    taken_hbm,
    change_hbm,
    final,
    grad,
    pool,
    summed,
    even,
    odd,
    models,
    source,
    wavelet,
    sums,
    part,
    gathered,
    product_out,
    product_in,
    send_sem,
    inner_sem,
    outer_sem,
    product_sem,
    part_sem,
):
    me = lax.axis_index("gz")
    rows, cols = grad.shape[1], grad.shape[2]
    chunks = rows // size
    tiles = size // 8
    upper = lax.rem(me, 2)
    has_outer = (me > 0) & (me < n - 1)
    inside = pl.ds(PAD, rows)
    chained = n - 1 <= steps
    inner_target = me + 1 - 2 * upper
    outer_target = lax.rem(me + n - 1 + 2 * upper, n)
    inner_plane, outer_plane = 2 - upper, 1 + upper
    inner_halo, outer_halo = 3 - 3 * upper, 3 * upper
    early = relayed * upper
    late = relayed - early
    lame, shear, coeff, prior = (models.at[i] for i in range(4))
    taken, change = pool.at[pl.ds(0, pairs)], pool.at[pl.ds(pairs, pairs)]

    barrier = pltpu.get_barrier_semaphore()

    def greet(device):
        pl.semaphore_signal(
            barrier, inc=1, device_id={"gz": device}, device_id_type=pl.DeviceIdType.MESH
        )

    if chained:

        @pl.when(has_outer)
        def _():
            greet(outer_target)

        greet(inner_target)
    else:
        for k in range(1, n):
            greet(lax.rem(me + k, n))

    loads = [
        pltpu.make_async_copy(src, dst, sem)
        for sem, src, dst in (
            (
                outer_sem.at[1, 0],
                now_hbm.at[:, :, pl.ds(0, size)],
                even.at[:, pl.ds(1, 2), pl.ds(PAD, size)],
            ),
            (
                inner_sem.at[1],
                now_hbm.at[:, :, pl.ds(size, rows - size)],
                even.at[:, pl.ds(1, 2), pl.ds(PAD + size, rows - size)],
            ),
            (product_sem.at[0], lame_hbm, lame),
            (product_sem.at[0], shear_hbm, shear),
            (product_sem.at[0], density_hbm, coeff),
            (product_sem.at[0], prior_hbm, prior),
            (product_sem.at[1], before_hbm, odd.at[:, pl.ds(1, 2), inside]),
            (part_sem.at[0], source_hbm, source),
            (send_sem.at[1], wavelet_hbm, wavelet),
            (part_sem.at[1], taken_hbm, taken),
            (part_sem.at[1], change_hbm, change),
        )
    ]
    for load in loads:
        load.start()

    def remote(src, dst, send, recv, target):
        return pltpu.make_async_remote_copy(
            src_ref=src,
            dst_ref=dst,
            send_sem=send,
            recv_sem=recv,
            device_id={"gz": target},
            device_id_type=pl.DeviceIdType.MESH,
        )

    def span(chunk):
        return pl.ds(pl.multiple_of(PAD + chunk * size, 8), size)

    def send_inner(ref, parity, chunk):
        remote(
            ref.at[:, inner_plane, span(chunk)],
            ref.at[:, 3 * upper, span(chunk)],
            send_sem.at[parity],
            inner_sem.at[parity],
            inner_target,
        ).start()

    def send_outer(ref, parity, chunk):
        remote(
            ref.at[:, outer_plane, span(chunk)],
            ref.at[:, 3 - 3 * upper, span(chunk)],
            send_sem.at[parity],
            outer_sem.at[parity, chunk],
            outer_target,
        ).start()

    def send(ref, parity, chunk):
        @pl.when(has_outer)
        def _():
            send_outer(ref, parity, chunk)

        send_inner(ref, parity, chunk)

    def sent(ref, parity):
        def wait(planes):
            whole_planes = ref.at[:, planes, inside]
            remote(
                whole_planes, whole_planes, send_sem.at[parity], inner_sem.at[parity], inner_target
            ).wait_send()

        @pl.when(has_outer)
        def _():
            wait(pl.ds(1, 2))

        @pl.when(jnp.logical_not(has_outer))
        def _():
            wait(pl.ds(1, 1))

    def received_inner(ref, parity):
        halo = ref.at[:, inner_halo, inside]
        remote(halo, halo, send_sem.at[parity], inner_sem.at[parity], inner_target).wait_recv()

    def received_outer(ref, parity, chunk):
        halo = ref.at[:, outer_halo, span(chunk)]
        remote(
            halo, halo, send_sem.at[parity], outer_sem.at[parity, chunk], outer_target
        ).wait_recv()

    loads[0].wait()
    if chained:
        pl.semaphore_wait(barrier, 1 + has_outer.astype(jnp.int32))
    else:
        pl.semaphore_wait(barrier, n - 1)

    send(even, 0, 0)
    loads[1].wait()

    def first(chunk, carry):
        send(even, 0, chunk)
        return carry

    lax.fori_loop(1, chunks, first, 0)

    edge = jnp.zeros((even.shape[0], 4, PAD, cols), jnp.float32)
    for ref in (even, odd):
        ref[:, :, pl.ds(0, PAD)] = edge
        ref[:, :, pl.ds(PAD + rows, PAD)] = edge

    @pl.when(jnp.logical_not(has_outer))
    def _():
        def body(t, carry):
            for ref in (even, odd):
                for comp in range(3):
                    ref[comp, outer_halo, tile(PAD + 8 * t)] = jnp.zeros((8, cols), jnp.float32)
            return carry

        lax.fori_loop(0, rows // 8, body, 0)

    pltpu.make_async_copy(models, models, product_sem.at[0]).wait()

    def prepare(t, carry):
        for plane in range(2):
            at = (plane, tile(8 * t))
            lame[at] = lame[at] + shear[at]
            coeff[at] = 0.04 / coeff[at]
            grad[at] = jnp.zeros((8, cols), jnp.float32)
        return carry

    lax.fori_loop(0, rows // 8, prepare, 0)
    for load in loads[6:9]:
        load.wait()
    pltpu.make_async_copy(pool, pool, part_sem.at[1]).wait()

    products = product_pairs(pairs)
    count = len(products)

    def stored(t, totals):
        totals = list(totals)
        for plane in range(2):
            vectors = [pool[i, plane, tile(8 * t)] for i in range(2 * pairs)]
            for k, (a, b) in enumerate(products):
                totals[k] = totals[k] + fold(vectors[a] * vectors[b])
        return tuple(totals)

    totals = lax.fori_loop(
        0, rows // 8, stored, tuple(jnp.zeros((8, 128), jnp.float32) for _ in products)
    )
    place = lax.broadcasted_iota(jnp.int32, (1, 128), 1)

    line = jnp.zeros((1, 128), jnp.float32)
    for k in range(count):
        line = jnp.where(place == k, whole(totals[k]), line)
    part[...] = line

    row_at = lax.broadcasted_iota(jnp.int32, (8, cols), 0)
    col_at = lax.broadcasted_iota(jnp.int32, (8, cols), 1)
    is_top, is_bottom = row_at == 0, row_at == 7
    is_left, is_right = col_at == 0, col_at == cols - 1

    def along_x(previous, value, following):
        minus = pltpu.roll(jnp.where(is_bottom, previous, value), 1, 0)
        plus = pltpu.roll(jnp.where(is_top, following, value), 7, 0)
        return minus, plus

    def along_y(value):
        minus = jnp.where(is_left, 0.0, pltpu.roll(value, 1, 1))
        plus = jnp.where(is_right, 0.0, pltpu.roll(value, cols - 1, 1))
        return minus, plus

    def delta_y(value):
        minus, plus = along_y(value)
        return plus - minus

    def update(step, current, other, t, last=False):
        amplitude = wavelet[step]

        def load(comp, plane, shift=0):
            return current[comp, plane, tile(PAD + 8 * (t + shift))]

        for plane in range(2):
            low, mid, high = plane, plane + 1, plane + 2
            at = tile(8 * t)
            here = tile(PAD + 8 * t)

            def delta_z(comp, shift=0):
                return load(comp, high, shift) - load(comp, low, shift)

            def delta_xz(comp, centre):
                minus, plus = along_x(delta_z(comp, -1), centre, delta_z(comp, 1))
                return plus - minus

            centre = [load(comp, mid) for comp in range(3)]
            diff = [delta_z(comp) for comp in range(3)]
            total = [load(comp, high) + load(comp, low) for comp in range(3)]
            xs = [along_x(load(comp, mid, -1), centre[comp], load(comp, mid, 1)) for comp in range(3)]
            ys = [along_y(centre[comp]) for comp in range(3)]
            sum_x = [minus + plus for minus, plus in xs]
            sum_y = [minus + plus for minus, plus in ys]
            dx = [plus - minus for minus, plus in xs]
            lap = [
                (total[comp] + sum_x[comp]) + (sum_y[comp] - 6.0 * centre[comp])
                for comp in range(3)
            ]
            mixed = [
                delta_xz(1, diff[1]) + delta_y(diff[2]),
                delta_xz(0, diff[0]) + delta_y(dx[2]),
                delta_y(diff[0] + dx[1]),
            ]
            own = [total[0], sum_x[1], sum_y[2]]
            both = lame[plane, at]
            mu = shear[plane, at]
            rate = coeff[plane, at]
            if not last:
                grad[plane, at] = grad[plane, at] + (
                    centre[0] * lap[0] + centre[1] * lap[1] + centre[2] * lap[2]
                )
            for comp in range(3):
                doubled = 2.0 * centre[comp]
                elastic = both * ((own[comp] - doubled) + 0.25 * mixed[comp]) + mu * lap[comp]
                value = (
                    doubled
                    - other[comp, mid, here]
                    + rate * (elastic + amplitude * source[comp, plane, at])
                )
                if last:
                    final[comp, plane, at] = value
                else:
                    other[comp, mid, here] = value

    def over_tiles(chunk, body):
        def tile_body(t, carry):
            body(chunk * tiles + t)
            return carry

        lax.fori_loop(0, tiles, tile_body, 0)

    def wait_outer(ref, parity, chunk):
        @pl.when(has_outer)
        def _():
            received_outer(ref, parity, chunk)

    def advance(step, current, other, parity, relay):
        @pl.when(step > 0)
        def _():
            sent(other, 1 - parity)

        received_inner(current, parity)
        wait_outer(current, parity, 0)

        def chunk_body(chunk, carry):
            @pl.when(chunk + 1 < chunks)
            def _():
                wait_outer(current, parity, chunk + 1)

            over_tiles(chunk, lambda t: update(step, current, other, t))
            if relay:

                @pl.when(has_outer & ((chunk < early) | (chunk >= early + relayed)))
                def _():
                    send_outer(other, 1 - parity, chunk)

                send_inner(other, 1 - parity, chunk)
            else:
                send(other, 1 - parity, chunk)
            return carry

        lax.fori_loop(0, chunks, chunk_body, 0)

    def two_steps(k, carry):
        advance(2 * k, even, odd, 0, False)
        advance(2 * k + 1, odd, even, 1, False)
        return carry

    lax.fori_loop(0, steps // 2 - 1, two_steps, 0)
    advance(steps - 2, even, odd, 0, True)

    def across(t):
        here = tile(PAD + 8 * t)
        value = odd[0, outer_plane, here] * odd[0, outer_halo, here]
        for comp in range(1, 3):
            value = value + odd[comp, outer_plane, here] * odd[comp, outer_halo, here]
        return value

    def returned(first, number, sem):
        where = pl.ds(first * size, number * size)
        return remote(
            product_out.at[where],
            product_in.at[where],
            product_sem.at[0],
            product_sem.at[sem],
            outer_target,
        )

    pieces = [(0, relayed - 1, 1), (relayed - 1, 1, 2)] if relayed > 1 else [(0, relayed, 1)]
    pieces = [piece for piece in pieces if piece[1]]
    if pieces:

        @pl.when(has_outer)
        def _():
            def multiply(chunk, carry):
                received_outer(odd, 1, early + chunk)
                for k in range(tiles):
                    t = chunk * tiles + k
                    product_out[tile(8 * t)] = across(early * tiles + t)
                return carry

            for piece in pieces:
                lax.fori_loop(piece[0], piece[0] + piece[1], multiply, 0)
                returned(*piece).start()

            def follow(chunk, carry):
                send_outer(odd, 1, early + chunk)
                return carry

            lax.fori_loop(0, relayed, follow, 0)

    received_inner(odd, 1)

    def weigh(totals, at, value):
        return tuple(
            totals[i] + fold(pool[(i,) + at] * value) for i in range(2 * pairs)
        )

    def own_part(t, totals):
        def load(comp, plane, shift=0):
            return odd[comp, plane, tile(PAD + 8 * (t + shift))]

        for mid, around in ((inner_plane, (outer_plane, inner_halo)), (outer_plane, (inner_plane,))):
            at = (mid - 1, tile(8 * t))
            value = None
            for comp in range(3):
                centre = load(comp, mid)
                minus_x, plus_x = along_x(load(comp, mid, -1), centre, load(comp, mid, 1))
                minus_y, plus_y = along_y(centre)
                total = load(comp, around[0])
                for plane in around[1:]:
                    total = total + load(comp, plane)
                lap = (total + (minus_x + plus_x)) + ((minus_y + plus_y) - 6.0 * centre)
                value = centre * lap if value is None else value + centre * lap
            value = (shear[at] - prior[at]) + 0.02 * (grad[at] + value)
            grad[at] = value
            totals = weigh(totals, at, value)
        return totals

    totals = lax.fori_loop(
        0,
        rows // 8,
        own_part,
        tuple(jnp.zeros((8, 128), jnp.float32) for _ in range(2 * pairs)),
        unroll=2,
    )
    for i in range(2 * pairs):
        sums[i] = totals[i]

    @pl.when(has_outer)
    def _():
        def add(t, product, totals):
            at = (outer_plane - 1, tile(8 * t))
            value = 0.02 * product
            grad[at] = grad[at] + value
            return weigh(totals, at, value)

        def added(products, start):
            return lambda t, totals: add(start * tiles + t, products[tile(8 * t)], totals)

        totals = tuple(sums[i] for i in range(2 * pairs))
        if relayed:
            totals = lax.fori_loop(0, relayed * tiles, added(product_out, early), totals)

        def direct(chunk, totals):
            received_outer(odd, 1, chunk)
            for k in range(tiles):
                t = chunk * tiles + k
                totals = add(t, across(t), totals)
            return totals

        totals = lax.fori_loop(2 * relayed, chunks, direct, totals)
        for piece in pieces:
            returned(*piece).wait_recv()
            totals = lax.fori_loop(
                piece[0] * tiles,
                (piece[0] + piece[1]) * tiles,
                added(product_in, late),
                totals,
                unroll=tiles,
            )
        for i in range(2 * pairs):
            sums[i] = totals[i]

    line = part[...]
    for i in range(2 * pairs):
        line = jnp.where(place == count + i, whole(sums[i]), line)
    part[...] = line

    def exchange(src, dst, target):
        return remote(src, dst, part_sem.at[0], part_sem.at[1], target)

    for target in range(n):

        @pl.when(me != target)
        def _():
            exchange(part, gathered.at[me], target).start()

    gathered[me] = line

    def close(chunk, carry):
        over_tiles(chunk, lambda t: update(steps - 1, odd, even, t, True))
        return carry

    ready = min(2 * relayed + 1, chunks) if relayed else 0
    lax.fori_loop(ready, chunks, close, 0)
    if relayed:

        @pl.when(has_outer)
        def _():
            def arrive(chunk, carry):
                received_outer(odd, 1, late + chunk)
                return carry

            lax.fori_loop(0, relayed, arrive, 0)

        lax.fori_loop(0, ready, close, 0)

        @pl.when(has_outer)
        def _():
            returned(0, relayed, 1).wait_send()

    sent(even, 0)
    sent(odd, 1)
    others = gathered.at[pl.ds(0, n - 1)]
    everything = exchange(others, others, inner_target)
    everything.wait_recv()
    line = gathered[0]
    for k in range(1, n):
        line = line + gathered[k]
    summed[...] = line
    everything.wait_send()


def publish(
    pairs,
    final,
    grad,
    pool,
    summed,
    final_hbm,
    grad_hbm,
    direction_hbm,
    direction,
    sem,
):
    rows, cols = grad.shape[1], grad.shape[2]
    copies = [
        pltpu.make_async_copy(final, final_hbm, sem.at[0]),
        pltpu.make_async_copy(grad, grad_hbm, sem.at[1]),
    ]
    for copy in copies:
        copy.start()

    place = lax.broadcasted_iota(jnp.int32, (1, 128), 1)
    products = product_pairs(pairs)
    count = len(products)
    where_of = {pair: k for k, pair in enumerate(products)}
    for i in range(2 * pairs):
        where_of[(i, 2 * pairs)] = count + i
    line = summed[...]
    cache = {}

    def inner(a, b):
        key = (min(a, b), max(a, b))
        if key not in cache:
            chosen = jnp.where(place == where_of[key], line, 0.0)
            cache[key] = jnp.sum(chosen, axis=1, keepdims=True)
        return cache[key]

    gradient_at = 2 * pairs
    curvature = [inner(i, pairs + i) for i in range(pairs)]
    alphas = [None] * pairs
    for i in reversed(range(pairs)):
        value = inner(i, gradient_at)
        for j in range(i + 1, pairs):
            value = value - alphas[j] * inner(i, pairs + j)
        alphas[i] = value / curvature[i]
    newest = 2 * pairs - 1
    gamma = curvature[pairs - 1] / inner(newest, newest)
    changes = [-gamma * alphas[i] for i in range(pairs)]
    steps_coef = [None] * pairs
    for i in range(pairs):
        value = gamma * inner(pairs + i, gradient_at)
        for j in range(pairs):
            value = value + changes[j] * inner(pairs + i, pairs + j)
        for j in range(i):
            value = value + steps_coef[j] * inner(j, pairs + i)
        steps_coef[i] = alphas[i] - value / curvature[i]

    def spread(value):
        return -jnp.broadcast_to(value, (8, cols))

    by_grad = spread(gamma)
    by_taken = [spread(value) for value in steps_coef]
    by_change = [spread(value) for value in changes]

    def combine(t, carry):
        for plane in range(2):
            at = (plane, tile(8 * t))
            value = by_grad * grad[at]
            for i in range(pairs):
                value = value + by_taken[i] * pool[(i,) + at]
                value = value + by_change[i] * pool[(pairs + i,) + at]
            direction[at] = value
        return carry

    tiles = rows // 8
    pieces = PIECES
    while tiles % pieces:
        pieces -= 1
    for piece in range(pieces):
        first, count = piece * (tiles // pieces), tiles // pieces
        lax.fori_loop(first, first + count, combine, 0, unroll=True)
        span = pl.ds(8 * first, 8 * count)
        copy = pltpu.make_async_copy(
            direction.at[:, span], direction_hbm.at[:, span], sem.at[2 + piece]
        )
        copy.start()
        copies.append(copy)
    for copy in copies:
        copy.wait()


def on_device(
    n,
    field_now,
    field_before,
    lame_lambda,
    shear_modulus,
    density,
    source_field,
    wavelet,
    prior_mean,
    steps_taken,
    grad_change,
):
    comps, depth, rows, cols = field_now.shape
    pairs = steps_taken.shape[0]
    steps = wavelet.shape[0]
    size = chunk_rows(rows)
    chunks = rows // size
    relayed = 3 * chunks // 10
    f32 = jnp.float32
    state = pltpu.VMEM((comps, depth + 2, rows + 2 * PAD, cols), f32)
    model = pltpu.VMEM((depth, rows, cols), f32)
    returned = pltpu.VMEM((max(relayed, 1) * size, cols), f32)
    dma = pltpu.SemaphoreType.DMA
    anywhere = pl.BlockSpec(memory_space=pltpu.HBM)
    free = pl.BlockSpec(memory_space=pl.ANY)
    in_vmem = pl.BlockSpec(memory_space=pltpu.VMEM)
    results = pl.pallas_call(
        functools.partial(kernel, n, steps, pairs, size, relayed),
        out_shape=(
            pltpu.VMEM(field_now.shape, f32),
            pltpu.VMEM(lame_lambda.shape, f32),
            pltpu.VMEM((2 * pairs,) + lame_lambda.shape, f32),
            pltpu.VMEM((1, 128), f32),
        ),
        in_specs=[anywhere] * 10,
        out_specs=(in_vmem,) * 4,
        scratch_shapes=[
            state,
            state,
            pltpu.VMEM((4, depth, rows, cols), f32),
            pltpu.VMEM((comps, depth, rows, cols), f32),
            pltpu.SMEM((steps,), f32),
            pltpu.VMEM((2 * pairs, 8, 128), f32),
            pltpu.VMEM((1, 128), f32),
            pltpu.VMEM((n, 1, 128), f32),
            returned,
            returned,
            dma((2,)),
            dma((2,)),
            dma((2, chunks)),
            dma((3,)),
            dma((2,)),
        ],
        compiler_params=pltpu.CompilerParams(
            collective_id=0, has_side_effects=True, vmem_limit_bytes=63000000
        ),
    )(
        field_now,
        field_before,
        lame_lambda,
        shear_modulus,
        density,
        source_field,
        wavelet,
        prior_mean,
        steps_taken,
        grad_change,
    )
    return pl.pallas_call(
        functools.partial(publish, pairs),
        out_shape=tuple(
            jax.ShapeDtypeStruct(shape, f32)
            for shape in (field_now.shape, lame_lambda.shape, lame_lambda.shape)
        ),
        in_specs=[in_vmem] * 4,
        out_specs=(free, free, free),
        scratch_shapes=[model, dma((2 + PIECES,))],
        compiler_params=pltpu.CompilerParams(vmem_limit_bytes=4 * 1024 * 1024),
    )(*[pltpu.with_memory_space_constraint(value, pltpu.VMEM) for value in results])


def solution(mesh):
    n = mesh.shape["gz"]
    fields = P("sample", "gz", None, None)
    models = P("gz", "sample", None)
    placed = (
        fields,
        fields,
        models,
        models,
        models,
        fields,
        P("sample"),
        models,
        fields,
        fields,
    )
    return jax.shard_map(
        functools.partial(on_device, n),
        mesh=mesh,
        in_specs=placed,
        out_specs=(fields, models, models),
        check_vma=False,
    )
```

```python
import functools

import jax
import jax.numpy as jnp
from jax import lax
from jax.experimental import pallas as pl
from jax.experimental.pallas import tpu as pltpu
from jax.sharding import PartitionSpec as P

PAD = 8
CHUNK_ROWS = 16
PIECES = 4
RELAY_AT = 1


def chunk_rows(rows):
    size = CHUNK_ROWS
    while rows % size:
        size //= 2
    return size


def tile(start):
    return pl.ds(pl.multiple_of(start, 8), 8)


def fold(value):
    out = value[:, 0:128]
    for k in range(1, value.shape[1] // 128):
        out = out + value[:, 128 * k : 128 * (k + 1)]
    return out


def whole(value):
    return jnp.sum(jnp.sum(value, axis=0, keepdims=True), axis=1, keepdims=True)


def product_pairs(pairs):
    found = [(i, pairs + j) for i in range(pairs) for j in range(pairs)]
    return found + [(pairs + i, pairs + j) for i in range(pairs) for j in range(i, pairs)]


def kernel(
    n,
    steps,
    pairs,
    size,
    relayed,
    helpers,
    now_hbm,
    before_hbm,
    lame_hbm,
    shear_hbm,
    density_hbm,
    source_hbm,
    wavelet_hbm,
    prior_hbm,
    taken_hbm,
    change_hbm,
    final,
    grad,
    pool,
    summed,
    even,
    odd,
    models,
    source,
    wavelet,
    sums,
    part,
    gathered,
    product_out,
    product_in,
    detour,
    send_sem,
    inner_sem,
    outer_sem,
    product_sem,
    part_sem,
    detour_sem,
    ready,
):
    me = lax.axis_index("gz")
    rows, cols = grad.shape[1], grad.shape[2]
    chunks = rows // size
    tiles = size // 8
    upper = lax.rem(me, 2)
    has_outer = (me > 0) & (me < n - 1)
    inside = pl.ds(PAD, rows)
    chained = n - 1 <= steps
    inner_target = me + 1 - 2 * upper
    outer_target = lax.rem(me + n - 1 + 2 * upper, n)
    inner_plane, outer_plane = 2 - upper, 1 + upper
    inner_halo, outer_halo = 3 - 3 * upper, 3 * upper
    early = relayed * upper
    late = relayed - early
    lame, shear, coeff, prior = (models.at[i] for i in range(4))
    taken, change = pool.at[pl.ds(0, pairs)], pool.at[pl.ds(pairs, pairs)]

    sample = lax.axis_index("sample")
    below, above = n - 3, n - 2
    assisted = (sample == 0) & ((me == below) | (me == above))
    helping = (sample >= 1) & (sample <= helpers)
    carries = helping & ((me == below - 1) | (me == above + 1))
    stripped = chunks - 1
    strip = pl.ds(PAD + stripped * size, size)

    barrier = pltpu.get_barrier_semaphore()

    def greet(device):
        pl.semaphore_signal(
            barrier, inc=1, device_id={"gz": device}, device_id_type=pl.DeviceIdType.MESH
        )

    def greet_across(semaphore, target_sample, device):
        pl.semaphore_signal(
            semaphore,
            inc=1,
            device_id={"sample": target_sample, "gz": device},
            device_id_type=pl.DeviceIdType.MESH,
        )

    if chained:

        @pl.when(has_outer)
        def _():
            greet(outer_target)

        greet(inner_target)
        if helpers:

            @pl.when(assisted)
            def _():
                for helper in range(1, helpers + 1):
                    greet_across(barrier, helper, inner_target)

    else:
        for k in range(1, n):
            greet(lax.rem(me + k, n))

    loads = [
        pltpu.make_async_copy(src, dst, sem)
        for sem, src, dst in (
            (
                outer_sem.at[1, 0],
                now_hbm.at[:, :, pl.ds(0, size)],
                even.at[:, pl.ds(1, 2), pl.ds(PAD, size)],
            ),
            (
                inner_sem.at[1],
                now_hbm.at[:, :, pl.ds(size, rows - size)],
                even.at[:, pl.ds(1, 2), pl.ds(PAD + size, rows - size)],
            ),
            (product_sem.at[0], lame_hbm, lame),
            (product_sem.at[0], shear_hbm, shear),
            (product_sem.at[0], density_hbm, coeff),
            (product_sem.at[0], prior_hbm, prior),
            (product_sem.at[1], before_hbm, odd.at[:, pl.ds(1, 2), inside]),
            (part_sem.at[0], source_hbm, source),
            (send_sem.at[1], wavelet_hbm, wavelet),
            (part_sem.at[1], taken_hbm, taken),
            (part_sem.at[1], change_hbm, change),
        )
    ]
    for load in loads:
        load.start()

    def remote(src, dst, send, recv, target, target_sample=None):
        device = {"gz": target}
        if target_sample is not None:
            device["sample"] = target_sample
        return pltpu.make_async_remote_copy(
            src_ref=src,
            dst_ref=dst,
            send_sem=send,
            recv_sem=recv,
            device_id=device,
            device_id_type=pl.DeviceIdType.MESH,
        )

    def span(chunk):
        return pl.ds(pl.multiple_of(PAD + chunk * size, 8), size)

    def send_inner(ref, parity, chunk):
        remote(
            ref.at[:, inner_plane, span(chunk)],
            ref.at[:, 3 * upper, span(chunk)],
            send_sem.at[parity],
            inner_sem.at[parity],
            inner_target,
        ).start()

    def send_outer(ref, parity, chunk):
        remote(
            ref.at[:, outer_plane, span(chunk)],
            ref.at[:, 3 - 3 * upper, span(chunk)],
            send_sem.at[parity],
            outer_sem.at[parity, chunk],
            outer_target,
        ).start()

    def send_strips(ref, parity):
        for helper in range(1, helpers + 1):
            remote(
                ref.at[helper - 1, outer_plane, strip],
                detour.at[parity],
                send_sem.at[parity],
                detour_sem.at[parity],
                inner_target,
                helper,
            ).start()

    def pass_on(ref, parity):
        return remote(
            detour.at[parity],
            ref.at[sample - 1, 3 * upper, strip],
            part_sem.at[0],
            detour_sem.at[parity],
            me + 2 - 4 * upper,
            0,
        )

    def received_strips(ref, parity):
        strips = ref.at[:, outer_halo, strip]
        remote(strips, strips, send_sem.at[parity], detour_sem.at[parity], outer_target).wait_recv()

    def send(ref, parity, chunk):
        @pl.when(has_outer)
        def _():
            send_outer(ref, parity, chunk)

        send_inner(ref, parity, chunk)

    def send_but_strips(ref, parity, chunk):
        @pl.when(has_outer & jnp.logical_not(assisted & (chunk >= stripped)))
        def _():
            send_outer(ref, parity, chunk)

        send_inner(ref, parity, chunk)

    def sent(ref, parity):
        def wait(planes):
            whole_planes = ref.at[:, planes, inside]
            remote(
                whole_planes, whole_planes, send_sem.at[parity], inner_sem.at[parity], inner_target
            ).wait_send()

        @pl.when(has_outer)
        def _():
            wait(pl.ds(1, 2))

        @pl.when(jnp.logical_not(has_outer))
        def _():
            wait(pl.ds(1, 1))

    def received_inner(ref, parity):
        halo = ref.at[:, inner_halo, inside]
        remote(halo, halo, send_sem.at[parity], inner_sem.at[parity], inner_target).wait_recv()

    def received_outer(ref, parity, chunk):
        halo = ref.at[:, outer_halo, span(chunk)]
        remote(
            halo, halo, send_sem.at[parity], outer_sem.at[parity, chunk], outer_target
        ).wait_recv()

    if chained:
        expected = 1 + has_outer.astype(jnp.int32)
        if helpers:
            expected = expected + carries.astype(jnp.int32)
        pl.semaphore_wait(barrier, expected)
    else:
        pl.semaphore_wait(barrier, n - 1)

    if helpers:

        @pl.when(carries)
        def _():
            greet_across(ready, 0, me + 1 - 2 * upper)

    loads[0].wait()
    send(even, 0, 0)
    loads[1].wait()

    def first(chunk, carry):
        (send_but_strips if helpers else send)(even, 0, chunk)
        return carry

    lax.fori_loop(1, chunks, first, 0)

    edge = jnp.zeros((even.shape[0], 4, PAD, cols), jnp.float32)
    for ref in (even, odd):
        ref[:, :, pl.ds(0, PAD)] = edge
        ref[:, :, pl.ds(PAD + rows, PAD)] = edge

    @pl.when(jnp.logical_not(has_outer))
    def _():
        def body(t, carry):
            for ref in (even, odd):
                for comp in range(3):
                    ref[comp, outer_halo, tile(PAD + 8 * t)] = jnp.zeros((8, cols), jnp.float32)
            return carry

        lax.fori_loop(0, rows // 8, body, 0)

    if helpers:

        @pl.when(assisted)
        def _():
            pl.semaphore_wait(ready, helpers)
            send_strips(even, 0)

    pltpu.make_async_copy(models, models, product_sem.at[0]).wait()

    def prepare(t, carry):
        for plane in range(2):
            at = (plane, tile(8 * t))
            lame[at] = lame[at] + shear[at]
            coeff[at] = 0.04 / coeff[at]
            grad[at] = jnp.zeros((8, cols), jnp.float32)
        return carry

    lax.fori_loop(0, rows // 8, prepare, 0)
    for load in loads[6:9]:
        load.wait()
    pltpu.make_async_copy(pool, pool, part_sem.at[1]).wait()

    products = product_pairs(pairs)
    count = len(products)

    def stored(t, totals):
        totals = list(totals)
        for plane in range(2):
            vectors = [pool[i, plane, tile(8 * t)] for i in range(2 * pairs)]
            for k, (a, b) in enumerate(products):
                totals[k] = totals[k] + fold(vectors[a] * vectors[b])
        return tuple(totals)

    totals = lax.fori_loop(
        0, rows // 8, stored, tuple(jnp.zeros((8, 128), jnp.float32) for _ in products)
    )
    place = lax.broadcasted_iota(jnp.int32, (1, 128), 1)

    line = jnp.zeros((1, 128), jnp.float32)
    for k in range(count):
        line = jnp.where(place == k, whole(totals[k]), line)
    part[...] = line

    row_at = lax.broadcasted_iota(jnp.int32, (8, cols), 0)
    col_at = lax.broadcasted_iota(jnp.int32, (8, cols), 1)
    is_top, is_bottom = row_at == 0, row_at == 7
    is_left, is_right = col_at == 0, col_at == cols - 1

    def along_x(previous, value, following):
        minus = pltpu.roll(jnp.where(is_bottom, previous, value), 1, 0)
        plus = pltpu.roll(jnp.where(is_top, following, value), 7, 0)
        return minus, plus

    def along_y(value):
        minus = jnp.where(is_left, 0.0, pltpu.roll(value, 1, 1))
        plus = jnp.where(is_right, 0.0, pltpu.roll(value, cols - 1, 1))
        return minus, plus

    def delta_y(value):
        minus, plus = along_y(value)
        return plus - minus

    def update(step, current, other, t, last=False):
        amplitude = wavelet[step]

        def load(comp, plane, shift=0):
            return current[comp, plane, tile(PAD + 8 * (t + shift))]

        for plane in range(2):
            low, mid, high = plane, plane + 1, plane + 2
            at = tile(8 * t)
            here = tile(PAD + 8 * t)

            def delta_z(comp, shift=0):
                return load(comp, high, shift) - load(comp, low, shift)

            def delta_xz(comp, centre):
                minus, plus = along_x(delta_z(comp, -1), centre, delta_z(comp, 1))
                return plus - minus

            centre = [load(comp, mid) for comp in range(3)]
            diff = [delta_z(comp) for comp in range(3)]
            total = [load(comp, high) + load(comp, low) for comp in range(3)]
            xs = [along_x(load(comp, mid, -1), centre[comp], load(comp, mid, 1)) for comp in range(3)]
            ys = [along_y(centre[comp]) for comp in range(3)]
            sum_x = [minus + plus for minus, plus in xs]
            sum_y = [minus + plus for minus, plus in ys]
            dx = [plus - minus for minus, plus in xs]
            lap = [
                (total[comp] + sum_x[comp]) + (sum_y[comp] - 6.0 * centre[comp])
                for comp in range(3)
            ]
            mixed = [
                delta_xz(1, diff[1]) + delta_y(diff[2]),
                delta_xz(0, diff[0]) + delta_y(dx[2]),
                delta_y(diff[0] + dx[1]),
            ]
            own = [total[0], sum_x[1], sum_y[2]]
            both = lame[plane, at]
            mu = shear[plane, at]
            rate = coeff[plane, at]
            if not last:
                grad[plane, at] = grad[plane, at] + (
                    centre[0] * lap[0] + centre[1] * lap[1] + centre[2] * lap[2]
                )
            for comp in range(3):
                doubled = 2.0 * centre[comp]
                elastic = both * ((own[comp] - doubled) + 0.25 * mixed[comp]) + mu * lap[comp]
                value = (
                    doubled
                    - other[comp, mid, here]
                    + rate * (elastic + amplitude * source[comp, plane, at])
                )
                if last:
                    final[comp, plane, at] = value
                else:
                    other[comp, mid, here] = value

    def over_tiles(chunk, body):
        def tile_body(t, carry):
            body(chunk * tiles + t)
            return carry

        lax.fori_loop(0, tiles, tile_body, 0)

    def wait_outer(ref, parity, chunk):
        @pl.when(has_outer)
        def _():
            received_outer(ref, parity, chunk)

    def wait_all_but_strips(ref, parity, chunk):
        @pl.when(assisted & (chunk == stripped))
        def _():
            received_strips(ref, parity)

        @pl.when(has_outer & jnp.logical_not(assisted & (chunk >= stripped)))
        def _():
            received_outer(ref, parity, chunk)

    def advance(step, current, other, parity, relay, detours=False):
        @pl.when(step > 0)
        def _():
            sent(other, 1 - parity)

        received_inner(current, parity)
        wait_outer(current, parity, 0)

        def chunk_body(chunk, carry):
            @pl.when(chunk + 1 < chunks)
            def _():
                (wait_all_but_strips if detours else wait_outer)(current, parity, chunk + 1)

            if detours:

                @pl.when(carries & (chunk == RELAY_AT))
                def _():
                    received = detour.at[parity]
                    remote(
                        received, received, part_sem.at[0], detour_sem.at[parity], inner_target
                    ).wait_recv()
                    pass_on(current, parity).start()

            over_tiles(chunk, lambda t: update(step, current, other, t))
            if relay:

                @pl.when(has_outer & ((chunk < early) | (chunk >= early + relayed)))
                def _():
                    send_outer(other, 1 - parity, chunk)

                send_inner(other, 1 - parity, chunk)
            else:
                send(other, 1 - parity, chunk)
            return carry

        lax.fori_loop(0, chunks, chunk_body, 0)

    def two_steps(k, carry):
        advance(2 * k, even, odd, 0, False)
        advance(2 * k + 1, odd, even, 1, False)
        return carry

    if helpers:
        advance(0, even, odd, 0, False, True)

        @pl.when(carries)
        def _():
            pass_on(even, 0).wait_send()

        advance(1, odd, even, 1, False)

    lax.fori_loop(1 if helpers else 0, steps // 2 - 1, two_steps, 0)
    advance(steps - 2, even, odd, 0, True)

    def across(t):
        here = tile(PAD + 8 * t)
        value = odd[0, outer_plane, here] * odd[0, outer_halo, here]
        for comp in range(1, 3):
            value = value + odd[comp, outer_plane, here] * odd[comp, outer_halo, here]
        return value

    def returned(first, number, sem):
        where = pl.ds(first * size, number * size)
        return remote(
            product_out.at[where],
            product_in.at[where],
            product_sem.at[0],
            product_sem.at[sem],
            outer_target,
        )

    pieces = [(0, relayed - 1, 1), (relayed - 1, 1, 2)] if relayed > 1 else [(0, relayed, 1)]
    pieces = [piece for piece in pieces if piece[1]]
    if pieces:

        @pl.when(has_outer)
        def _():
            def multiply(chunk, carry):
                received_outer(odd, 1, early + chunk)
                for k in range(tiles):
                    t = chunk * tiles + k
                    product_out[tile(8 * t)] = across(early * tiles + t)
                return carry

            for piece in pieces:
                lax.fori_loop(piece[0], piece[0] + piece[1], multiply, 0)
                returned(*piece).start()

            def follow(chunk, carry):
                send_outer(odd, 1, early + chunk)
                return carry

            lax.fori_loop(0, relayed, follow, 0)

    received_inner(odd, 1)

    def weigh(totals, at, value):
        return tuple(
            totals[i] + fold(pool[(i,) + at] * value) for i in range(2 * pairs)
        )

    def own_part(t, totals):
        def load(comp, plane, shift=0):
            return odd[comp, plane, tile(PAD + 8 * (t + shift))]

        for mid, around in ((inner_plane, (outer_plane, inner_halo)), (outer_plane, (inner_plane,))):
            at = (mid - 1, tile(8 * t))
            value = None
            for comp in range(3):
                centre = load(comp, mid)
                minus_x, plus_x = along_x(load(comp, mid, -1), centre, load(comp, mid, 1))
                minus_y, plus_y = along_y(centre)
                total = load(comp, around[0])
                for plane in around[1:]:
                    total = total + load(comp, plane)
                lap = (total + (minus_x + plus_x)) + ((minus_y + plus_y) - 6.0 * centre)
                value = centre * lap if value is None else value + centre * lap
            value = (shear[at] - prior[at]) + 0.02 * (grad[at] + value)
            grad[at] = value
            totals = weigh(totals, at, value)
        return totals

    totals = lax.fori_loop(
        0,
        rows // 8,
        own_part,
        tuple(jnp.zeros((8, 128), jnp.float32) for _ in range(2 * pairs)),
        unroll=2,
    )
    for i in range(2 * pairs):
        sums[i] = totals[i]

    @pl.when(has_outer)
    def _():
        def add(t, product, totals):
            at = (outer_plane - 1, tile(8 * t))
            value = 0.02 * product
            grad[at] = grad[at] + value
            return weigh(totals, at, value)

        def added(products, start):
            return lambda t, totals: add(start * tiles + t, products[tile(8 * t)], totals)

        totals = tuple(sums[i] for i in range(2 * pairs))
        if relayed:
            totals = lax.fori_loop(0, relayed * tiles, added(product_out, early), totals)

        def direct(chunk, totals):
            received_outer(odd, 1, chunk)
            for k in range(tiles):
                t = chunk * tiles + k
                totals = add(t, across(t), totals)
            return totals

        totals = lax.fori_loop(2 * relayed, chunks, direct, totals)
        for piece in pieces:
            returned(*piece).wait_recv()
            totals = lax.fori_loop(
                piece[0] * tiles,
                (piece[0] + piece[1]) * tiles,
                added(product_in, late),
                totals,
                unroll=tiles,
            )
        for i in range(2 * pairs):
            sums[i] = totals[i]

    line = part[...]
    for i in range(2 * pairs):
        line = jnp.where(place == count + i, whole(sums[i]), line)
    part[...] = line

    def exchange(src, dst, target):
        return remote(src, dst, part_sem.at[0], part_sem.at[1], target)

    for target in range(n):

        @pl.when(me != target)
        def _():
            exchange(part, gathered.at[me], target).start()

    gathered[me] = line

    def close(chunk, carry):
        over_tiles(chunk, lambda t: update(steps - 1, odd, even, t, True))
        return carry

    ready = min(2 * relayed + 1, chunks) if relayed else 0
    lax.fori_loop(ready, chunks, close, 0)
    if relayed:

        @pl.when(has_outer)
        def _():
            def arrive(chunk, carry):
                received_outer(odd, 1, late + chunk)
                return carry

            lax.fori_loop(0, relayed, arrive, 0)

        lax.fori_loop(0, ready, close, 0)

        @pl.when(has_outer)
        def _():
            returned(0, relayed, 1).wait_send()

    sent(even, 0)
    sent(odd, 1)
    others = gathered.at[pl.ds(0, n - 1)]
    everything = exchange(others, others, inner_target)
    everything.wait_recv()
    line = gathered[0]
    for k in range(1, n):
        line = line + gathered[k]
    summed[...] = line
    everything.wait_send()


def publish(
    pairs,
    final,
    grad,
    pool,
    summed,
    final_hbm,
    grad_hbm,
    direction_hbm,
    direction,
    sem,
):
    rows, cols = grad.shape[1], grad.shape[2]
    copies = [
        pltpu.make_async_copy(final, final_hbm, sem.at[0]),
        pltpu.make_async_copy(grad, grad_hbm, sem.at[1]),
    ]
    for copy in copies:
        copy.start()

    place = lax.broadcasted_iota(jnp.int32, (1, 128), 1)
    products = product_pairs(pairs)
    count = len(products)
    where_of = {pair: k for k, pair in enumerate(products)}
    for i in range(2 * pairs):
        where_of[(i, 2 * pairs)] = count + i
    line = summed[...]
    cache = {}

    def inner(a, b):
        key = (min(a, b), max(a, b))
        if key not in cache:
            chosen = jnp.where(place == where_of[key], line, 0.0)
            cache[key] = jnp.sum(chosen, axis=1, keepdims=True)
        return cache[key]

    gradient_at = 2 * pairs
    curvature = [inner(i, pairs + i) for i in range(pairs)]
    alphas = [None] * pairs
    for i in reversed(range(pairs)):
        value = inner(i, gradient_at)
        for j in range(i + 1, pairs):
            value = value - alphas[j] * inner(i, pairs + j)
        alphas[i] = value / curvature[i]
    newest = 2 * pairs - 1
    gamma = curvature[pairs - 1] / inner(newest, newest)
    changes = [-gamma * alphas[i] for i in range(pairs)]
    steps_coef = [None] * pairs
    for i in range(pairs):
        value = gamma * inner(pairs + i, gradient_at)
        for j in range(pairs):
            value = value + changes[j] * inner(pairs + i, pairs + j)
        for j in range(i):
            value = value + steps_coef[j] * inner(j, pairs + i)
        steps_coef[i] = alphas[i] - value / curvature[i]

    def spread(value):
        return -jnp.broadcast_to(value, (8, cols))

    by_grad = spread(gamma)
    by_taken = [spread(value) for value in steps_coef]
    by_change = [spread(value) for value in changes]

    def combine(t, carry):
        for plane in range(2):
            at = (plane, tile(8 * t))
            value = by_grad * grad[at]
            for i in range(pairs):
                value = value + by_taken[i] * pool[(i,) + at]
                value = value + by_change[i] * pool[(pairs + i,) + at]
            direction[at] = value
        return carry

    tiles = rows // 8
    pieces = PIECES
    while tiles % pieces:
        pieces -= 1
    for piece in range(pieces):
        first, count = piece * (tiles // pieces), tiles // pieces
        lax.fori_loop(first, first + count, combine, 0, unroll=True)
        span = pl.ds(8 * first, 8 * count)
        copy = pltpu.make_async_copy(
            direction.at[:, span], direction_hbm.at[:, span], sem.at[2 + piece]
        )
        copy.start()
        copies.append(copy)
    for copy in copies:
        copy.wait()


def on_device(
    n,
    samples,
    field_now,
    field_before,
    lame_lambda,
    shear_modulus,
    density,
    source_field,
    wavelet,
    prior_mean,
    steps_taken,
    grad_change,
):
    comps, depth, rows, cols = field_now.shape
    pairs = steps_taken.shape[0]
    steps = wavelet.shape[0]
    size = chunk_rows(rows)
    chunks = rows // size
    relayed = 3 * chunks // 10
    assist = samples > comps and 8 <= n <= steps + 1 and steps >= 6 and chunks > 4
    helpers = comps if assist else 0
    f32 = jnp.float32
    state = pltpu.VMEM((comps, depth + 2, rows + 2 * PAD, cols), f32)
    model = pltpu.VMEM((depth, rows, cols), f32)
    returned = pltpu.VMEM((max(relayed, 1) * size, cols), f32)
    dma = pltpu.SemaphoreType.DMA
    anywhere = pl.BlockSpec(memory_space=pltpu.HBM)
    free = pl.BlockSpec(memory_space=pl.ANY)
    in_vmem = pl.BlockSpec(memory_space=pltpu.VMEM)
    results = pl.pallas_call(
        functools.partial(kernel, n, steps, pairs, size, relayed, helpers),
        out_shape=(
            pltpu.VMEM(field_now.shape, f32),
            pltpu.VMEM(lame_lambda.shape, f32),
            pltpu.VMEM((2 * pairs,) + lame_lambda.shape, f32),
            pltpu.VMEM((1, 128), f32),
        ),
        in_specs=[anywhere] * 10,
        out_specs=(in_vmem,) * 4,
        scratch_shapes=[
            state,
            state,
            pltpu.VMEM((4, depth, rows, cols), f32),
            pltpu.VMEM((comps, depth, rows, cols), f32),
            pltpu.SMEM((steps,), f32),
            pltpu.VMEM((2 * pairs, 8, 128), f32),
            pltpu.VMEM((1, 128), f32),
            pltpu.VMEM((n, 1, 128), f32),
            returned,
            returned,
            pltpu.VMEM((1, size, cols), f32),
            dma((2,)),
            dma((2,)),
            dma((2, chunks)),
            dma((3,)),
            dma((2,)),
            dma((1,)),
            pltpu.SemaphoreType.REGULAR,
        ],
        compiler_params=pltpu.CompilerParams(
            collective_id=0, has_side_effects=True, vmem_limit_bytes=63000000
        ),
    )(
        field_now,
        field_before,
        lame_lambda,
        shear_modulus,
        density,
        source_field,
        wavelet,
        prior_mean,
        steps_taken,
        grad_change,
    )
    return pl.pallas_call(
        functools.partial(publish, pairs),
        out_shape=tuple(
            jax.ShapeDtypeStruct(shape, f32)
            for shape in (field_now.shape, lame_lambda.shape, lame_lambda.shape)
        ),
        in_specs=[in_vmem] * 4,
        out_specs=(free, free, free),
        scratch_shapes=[model, dma((2 + PIECES,))],
        compiler_params=pltpu.CompilerParams(vmem_limit_bytes=4 * 1024 * 1024),
    )(*[pltpu.with_memory_space_constraint(value, pltpu.VMEM) for value in results])


def solution(mesh):
    n = mesh.shape["gz"]
    fields = P("sample", "gz", None, None)
    models = P("gz", "sample", None)
    placed = (
        fields,
        fields,
        models,
        models,
        models,
        fields,
        P("sample"),
        models,
        fields,
        fields,
    )
    return jax.shard_map(
        functools.partial(on_device, n, mesh.shape["sample"]),
        mesh=mesh,
        in_specs=placed,
        out_specs=(fields, models, models),
        check_vma=False,
    )
```

```python
import functools

import jax
import jax.numpy as jnp
from jax import lax
from jax.experimental import pallas as pl
from jax.experimental.pallas import tpu as pltpu
from jax.sharding import PartitionSpec as P

PAD = 8
CHUNK_ROWS = 16
PIECES = 4
RELAY_AT = 1


def chunk_rows(rows):
    size = CHUNK_ROWS
    while rows % size:
        size //= 2
    return size


def tile(start):
    return pl.ds(pl.multiple_of(start, 8), 8)


def fold(value):
    out = value[:, 0:128]
    for k in range(1, value.shape[1] // 128):
        out = out + value[:, 128 * k : 128 * (k + 1)]
    return out


def whole(value):
    return jnp.sum(jnp.sum(value, axis=0, keepdims=True), axis=1, keepdims=True)


def product_pairs(pairs):
    found = [(i, pairs + j) for i in range(pairs) for j in range(pairs)]
    return found + [(pairs + i, pairs + j) for i in range(pairs) for j in range(i, pairs)]


def kernel(
    n,
    steps,
    pairs,
    size,
    relayed,
    helpers,
    now_hbm,
    before_hbm,
    lame_hbm,
    shear_hbm,
    density_hbm,
    source_hbm,
    wavelet_hbm,
    prior_hbm,
    taken_hbm,
    change_hbm,
    final,
    grad,
    pool,
    summed,
    even,
    odd,
    models,
    source,
    wavelet,
    sums,
    part,
    gathered,
    product_out,
    product_in,
    detour,
    send_sem,
    inner_sem,
    outer_sem,
    product_sem,
    part_sem,
    detour_sem,
    ready,
):
    me = lax.axis_index("gz")
    rows, cols = grad.shape[1], grad.shape[2]
    chunks = rows // size
    tiles = size // 8
    upper = lax.rem(me, 2)
    has_outer = (me > 0) & (me < n - 1)
    inside = pl.ds(PAD, rows)
    chained = n - 1 <= steps
    inner_target = me + 1 - 2 * upper
    outer_target = lax.rem(me + n - 1 + 2 * upper, n)
    inner_plane, outer_plane = 2 - upper, 1 + upper
    inner_halo, outer_halo = 3 - 3 * upper, 3 * upper
    early = relayed * upper
    late = relayed - early
    lame, shear, coeff, prior = (models.at[i] for i in range(4))
    taken, change = pool.at[pl.ds(0, pairs)], pool.at[pl.ds(pairs, pairs)]

    sample = lax.axis_index("sample")
    below, above = n - 3, n - 2
    assisted = (sample == 0) & ((me == below) | (me == above))
    helping = (sample >= 1) & (sample <= helpers)
    carries = helping & ((me == below - 1) | (me == above + 1))
    stripped = chunks - 2
    strip = pl.ds(PAD + stripped * size, 2 * size)

    barrier = pltpu.get_barrier_semaphore()

    def greet(device):
        pl.semaphore_signal(
            barrier, inc=1, device_id={"gz": device}, device_id_type=pl.DeviceIdType.MESH
        )

    def greet_across(semaphore, target_sample, device):
        pl.semaphore_signal(
            semaphore,
            inc=1,
            device_id={"sample": target_sample, "gz": device},
            device_id_type=pl.DeviceIdType.MESH,
        )

    if chained:

        @pl.when(has_outer)
        def _():
            greet(outer_target)

        greet(inner_target)
        if helpers:

            @pl.when(assisted)
            def _():
                for helper in range(1, helpers + 1):
                    greet_across(barrier, helper, inner_target)

    else:
        for k in range(1, n):
            greet(lax.rem(me + k, n))

    loads = [
        pltpu.make_async_copy(src, dst, sem)
        for sem, src, dst in (
            (
                outer_sem.at[1, 0],
                now_hbm.at[:, :, pl.ds(0, size)],
                even.at[:, pl.ds(1, 2), pl.ds(PAD, size)],
            ),
            (
                inner_sem.at[1],
                now_hbm.at[:, :, pl.ds(size, rows - size)],
                even.at[:, pl.ds(1, 2), pl.ds(PAD + size, rows - size)],
            ),
            (product_sem.at[0], lame_hbm, lame),
            (product_sem.at[0], shear_hbm, shear),
            (product_sem.at[0], density_hbm, coeff),
            (product_sem.at[0], prior_hbm, prior),
            (product_sem.at[1], before_hbm, odd.at[:, pl.ds(1, 2), inside]),
            (part_sem.at[0], source_hbm, source),
            (send_sem.at[1], wavelet_hbm, wavelet),
            (part_sem.at[1], taken_hbm, taken),
            (part_sem.at[1], change_hbm, change),
        )
    ]
    for load in loads:
        load.start()

    def remote(src, dst, send, recv, target, target_sample=None):
        device = {"gz": target}
        if target_sample is not None:
            device["sample"] = target_sample
        return pltpu.make_async_remote_copy(
            src_ref=src,
            dst_ref=dst,
            send_sem=send,
            recv_sem=recv,
            device_id=device,
            device_id_type=pl.DeviceIdType.MESH,
        )

    def span(chunk):
        return pl.ds(pl.multiple_of(PAD + chunk * size, 8), size)

    def send_inner(ref, parity, chunk):
        remote(
            ref.at[:, inner_plane, span(chunk)],
            ref.at[:, 3 * upper, span(chunk)],
            send_sem.at[parity],
            inner_sem.at[parity],
            inner_target,
        ).start()

    def send_outer(ref, parity, chunk):
        remote(
            ref.at[:, outer_plane, span(chunk)],
            ref.at[:, 3 - 3 * upper, span(chunk)],
            send_sem.at[parity],
            outer_sem.at[parity, chunk],
            outer_target,
        ).start()

    def send_strips(ref, parity):
        for helper in range(1, helpers + 1):
            remote(
                ref.at[helper - 1, outer_plane, strip],
                detour.at[parity],
                send_sem.at[parity],
                detour_sem.at[parity],
                inner_target,
                helper,
            ).start()

    def pass_on(ref, parity):
        return remote(
            detour.at[parity],
            ref.at[sample - 1, 3 * upper, strip],
            part_sem.at[0],
            detour_sem.at[parity],
            me + 2 - 4 * upper,
            0,
        )

    def received_strips(ref, parity):
        strips = ref.at[pl.ds(0, helpers), outer_halo, strip]
        remote(strips, strips, send_sem.at[parity], detour_sem.at[parity], outer_target).wait_recv()

    def send(ref, parity, chunk):
        @pl.when(has_outer)
        def _():
            send_outer(ref, parity, chunk)

        send_inner(ref, parity, chunk)

    others = pl.ds(helpers, even.shape[0] - helpers)

    def send_but_strips(ref, parity, chunk):
        cut = assisted & (chunk >= stripped)

        @pl.when(has_outer & jnp.logical_not(cut))
        def _():
            send_outer(ref, parity, chunk)

        @pl.when(cut)
        def _():
            remote(
                ref.at[others, outer_plane, span(chunk)],
                ref.at[others, 3 - 3 * upper, span(chunk)],
                send_sem.at[parity],
                outer_sem.at[parity, chunk],
                outer_target,
            ).start()

        send_inner(ref, parity, chunk)

    def sent(ref, parity):
        def wait(planes):
            whole_planes = ref.at[:, planes, inside]
            remote(
                whole_planes, whole_planes, send_sem.at[parity], inner_sem.at[parity], inner_target
            ).wait_send()

        @pl.when(has_outer)
        def _():
            wait(pl.ds(1, 2))

        @pl.when(jnp.logical_not(has_outer))
        def _():
            wait(pl.ds(1, 1))

    def received_inner(ref, parity):
        halo = ref.at[:, inner_halo, inside]
        remote(halo, halo, send_sem.at[parity], inner_sem.at[parity], inner_target).wait_recv()

    def received_outer(ref, parity, chunk):
        halo = ref.at[:, outer_halo, span(chunk)]
        remote(
            halo, halo, send_sem.at[parity], outer_sem.at[parity, chunk], outer_target
        ).wait_recv()

    if chained:
        expected = 1 + has_outer.astype(jnp.int32)
        if helpers:
            expected = expected + carries.astype(jnp.int32)
        pl.semaphore_wait(barrier, expected)
    else:
        pl.semaphore_wait(barrier, n - 1)

    if helpers:

        @pl.when(carries)
        def _():
            greet_across(ready, 0, me + 1 - 2 * upper)

    loads[0].wait()
    send(even, 0, 0)
    loads[1].wait()

    def first(chunk, carry):
        (send_but_strips if helpers else send)(even, 0, chunk)
        return carry

    lax.fori_loop(1, chunks, first, 0)

    edge = jnp.zeros((even.shape[0], 4, PAD, cols), jnp.float32)
    for ref in (even, odd):
        ref[:, :, pl.ds(0, PAD)] = edge
        ref[:, :, pl.ds(PAD + rows, PAD)] = edge

    @pl.when(jnp.logical_not(has_outer))
    def _():
        def body(t, carry):
            for ref in (even, odd):
                for comp in range(3):
                    ref[comp, outer_halo, tile(PAD + 8 * t)] = jnp.zeros((8, cols), jnp.float32)
            return carry

        lax.fori_loop(0, rows // 8, body, 0)

    if helpers:

        @pl.when(assisted)
        def _():
            pl.semaphore_wait(ready, helpers)
            send_strips(even, 0)

    pltpu.make_async_copy(models, models, product_sem.at[0]).wait()

    def prepare(t, carry):
        for plane in range(2):
            at = (plane, tile(8 * t))
            lame[at] = lame[at] + shear[at]
            coeff[at] = 0.04 / coeff[at]
            grad[at] = jnp.zeros((8, cols), jnp.float32)
        return carry

    lax.fori_loop(0, rows // 8, prepare, 0)
    for load in loads[6:9]:
        load.wait()
    pltpu.make_async_copy(pool, pool, part_sem.at[1]).wait()

    products = product_pairs(pairs)
    count = len(products)

    def stored(t, totals):
        totals = list(totals)
        for plane in range(2):
            vectors = [pool[i, plane, tile(8 * t)] for i in range(2 * pairs)]
            for k, (a, b) in enumerate(products):
                totals[k] = totals[k] + fold(vectors[a] * vectors[b])
        return tuple(totals)

    totals = lax.fori_loop(
        0, rows // 8, stored, tuple(jnp.zeros((8, 128), jnp.float32) for _ in products)
    )
    place = lax.broadcasted_iota(jnp.int32, (1, 128), 1)

    line = jnp.zeros((1, 128), jnp.float32)
    for k in range(count):
        line = jnp.where(place == k, whole(totals[k]), line)
    part[...] = line

    row_at = lax.broadcasted_iota(jnp.int32, (8, cols), 0)
    col_at = lax.broadcasted_iota(jnp.int32, (8, cols), 1)
    is_top, is_bottom = row_at == 0, row_at == 7
    is_left, is_right = col_at == 0, col_at == cols - 1

    def along_x(previous, value, following):
        minus = pltpu.roll(jnp.where(is_bottom, previous, value), 1, 0)
        plus = pltpu.roll(jnp.where(is_top, following, value), 7, 0)
        return minus, plus

    def along_y(value):
        minus = jnp.where(is_left, 0.0, pltpu.roll(value, 1, 1))
        plus = jnp.where(is_right, 0.0, pltpu.roll(value, cols - 1, 1))
        return minus, plus

    def delta_y(value):
        minus, plus = along_y(value)
        return plus - minus

    def update(step, current, other, t, last=False):
        amplitude = wavelet[step]

        def load(comp, plane, shift=0):
            return current[comp, plane, tile(PAD + 8 * (t + shift))]

        for plane in range(2):
            low, mid, high = plane, plane + 1, plane + 2
            at = tile(8 * t)
            here = tile(PAD + 8 * t)

            def delta_z(comp, shift=0):
                return load(comp, high, shift) - load(comp, low, shift)

            def delta_xz(comp, centre):
                minus, plus = along_x(delta_z(comp, -1), centre, delta_z(comp, 1))
                return plus - minus

            centre = [load(comp, mid) for comp in range(3)]
            diff = [delta_z(comp) for comp in range(3)]
            total = [load(comp, high) + load(comp, low) for comp in range(3)]
            xs = [along_x(load(comp, mid, -1), centre[comp], load(comp, mid, 1)) for comp in range(3)]
            ys = [along_y(centre[comp]) for comp in range(3)]
            sum_x = [minus + plus for minus, plus in xs]
            sum_y = [minus + plus for minus, plus in ys]
            dx = [plus - minus for minus, plus in xs]
            lap = [
                (total[comp] + sum_x[comp]) + (sum_y[comp] - 6.0 * centre[comp])
                for comp in range(3)
            ]
            mixed = [
                delta_xz(1, diff[1]) + delta_y(diff[2]),
                delta_xz(0, diff[0]) + delta_y(dx[2]),
                delta_y(diff[0] + dx[1]),
            ]
            own = [total[0], sum_x[1], sum_y[2]]
            both = lame[plane, at]
            mu = shear[plane, at]
            rate = coeff[plane, at]
            if not last:
                grad[plane, at] = grad[plane, at] + (
                    centre[0] * lap[0] + centre[1] * lap[1] + centre[2] * lap[2]
                )
            for comp in range(3):
                doubled = 2.0 * centre[comp]
                elastic = both * ((own[comp] - doubled) + 0.25 * mixed[comp]) + mu * lap[comp]
                value = (
                    doubled
                    - other[comp, mid, here]
                    + rate * (elastic + amplitude * source[comp, plane, at])
                )
                if last:
                    final[comp, plane, at] = value
                else:
                    other[comp, mid, here] = value

    def over_tiles(chunk, body):
        def tile_body(t, carry):
            body(chunk * tiles + t)
            return carry

        lax.fori_loop(0, tiles, tile_body, 0)

    def wait_outer(ref, parity, chunk):
        @pl.when(has_outer)
        def _():
            received_outer(ref, parity, chunk)

    def wait_all_but_strips(ref, parity, chunk):
        @pl.when(assisted & (chunk == stripped))
        def _():
            received_strips(ref, parity)

        @pl.when(has_outer & jnp.logical_not(assisted & (chunk >= stripped)))
        def _():
            received_outer(ref, parity, chunk)

        @pl.when(assisted & (chunk >= stripped))
        def _():
            rest = ref.at[others, outer_halo, span(chunk)]
            remote(
                rest, rest, send_sem.at[parity], outer_sem.at[parity, chunk], outer_target
            ).wait_recv()

    def advance(step, current, other, parity, relay, detours=False):
        @pl.when(step > 0)
        def _():
            sent(other, 1 - parity)

        received_inner(current, parity)
        wait_outer(current, parity, 0)

        def chunk_body(chunk, carry):
            @pl.when(chunk + 1 < chunks)
            def _():
                (wait_all_but_strips if detours else wait_outer)(current, parity, chunk + 1)

            if detours:

                @pl.when(carries & (chunk == RELAY_AT))
                def _():
                    received = detour.at[parity]
                    remote(
                        received, received, part_sem.at[0], detour_sem.at[parity], inner_target
                    ).wait_recv()
                    pass_on(current, parity).start()

            over_tiles(chunk, lambda t: update(step, current, other, t))
            if relay:

                @pl.when(has_outer & ((chunk < early) | (chunk >= early + relayed)))
                def _():
                    send_outer(other, 1 - parity, chunk)

                send_inner(other, 1 - parity, chunk)
            else:
                send(other, 1 - parity, chunk)
            return carry

        lax.fori_loop(0, chunks, chunk_body, 0)

    def two_steps(k, carry):
        advance(2 * k, even, odd, 0, False)
        advance(2 * k + 1, odd, even, 1, False)
        return carry

    if helpers:
        advance(0, even, odd, 0, False, True)

        @pl.when(carries)
        def _():
            pass_on(even, 0).wait_send()

        advance(1, odd, even, 1, False)

    lax.fori_loop(1 if helpers else 0, steps // 2 - 1, two_steps, 0)
    advance(steps - 2, even, odd, 0, True)

    def across(t):
        here = tile(PAD + 8 * t)
        value = odd[0, outer_plane, here] * odd[0, outer_halo, here]
        for comp in range(1, 3):
            value = value + odd[comp, outer_plane, here] * odd[comp, outer_halo, here]
        return value

    def returned(first, number, sem):
        where = pl.ds(first * size, number * size)
        return remote(
            product_out.at[where],
            product_in.at[where],
            product_sem.at[0],
            product_sem.at[sem],
            outer_target,
        )

    pieces = [(0, relayed - 1, 1), (relayed - 1, 1, 2)] if relayed > 1 else [(0, relayed, 1)]
    pieces = [piece for piece in pieces if piece[1]]
    if pieces:

        @pl.when(has_outer)
        def _():
            def multiply(chunk, carry):
                received_outer(odd, 1, early + chunk)
                for k in range(tiles):
                    t = chunk * tiles + k
                    product_out[tile(8 * t)] = across(early * tiles + t)
                return carry

            for piece in pieces:
                lax.fori_loop(piece[0], piece[0] + piece[1], multiply, 0)
                returned(*piece).start()

            def follow(chunk, carry):
                send_outer(odd, 1, early + chunk)
                return carry

            lax.fori_loop(0, relayed, follow, 0)

    received_inner(odd, 1)

    def weigh(totals, at, value):
        return tuple(
            totals[i] + fold(pool[(i,) + at] * value) for i in range(2 * pairs)
        )

    def own_part(t, totals):
        def load(comp, plane, shift=0):
            return odd[comp, plane, tile(PAD + 8 * (t + shift))]

        for mid, around in ((inner_plane, (outer_plane, inner_halo)), (outer_plane, (inner_plane,))):
            at = (mid - 1, tile(8 * t))
            value = None
            for comp in range(3):
                centre = load(comp, mid)
                minus_x, plus_x = along_x(load(comp, mid, -1), centre, load(comp, mid, 1))
                minus_y, plus_y = along_y(centre)
                total = load(comp, around[0])
                for plane in around[1:]:
                    total = total + load(comp, plane)
                lap = (total + (minus_x + plus_x)) + ((minus_y + plus_y) - 6.0 * centre)
                value = centre * lap if value is None else value + centre * lap
            value = (shear[at] - prior[at]) + 0.02 * (grad[at] + value)
            grad[at] = value
            totals = weigh(totals, at, value)
        return totals

    totals = lax.fori_loop(
        0,
        rows // 8,
        own_part,
        tuple(jnp.zeros((8, 128), jnp.float32) for _ in range(2 * pairs)),
        unroll=2,
    )
    for i in range(2 * pairs):
        sums[i] = totals[i]

    @pl.when(has_outer)
    def _():
        def add(t, product, totals):
            at = (outer_plane - 1, tile(8 * t))
            value = 0.02 * product
            grad[at] = grad[at] + value
            return weigh(totals, at, value)

        def added(products, start):
            return lambda t, totals: add(start * tiles + t, products[tile(8 * t)], totals)

        totals = tuple(sums[i] for i in range(2 * pairs))
        if relayed:
            totals = lax.fori_loop(0, relayed * tiles, added(product_out, early), totals)

        def direct(chunk, totals):
            received_outer(odd, 1, chunk)
            for k in range(tiles):
                t = chunk * tiles + k
                totals = add(t, across(t), totals)
            return totals

        totals = lax.fori_loop(2 * relayed, chunks, direct, totals)
        for piece in pieces:
            returned(*piece).wait_recv()
            totals = lax.fori_loop(
                piece[0] * tiles,
                (piece[0] + piece[1]) * tiles,
                added(product_in, late),
                totals,
                unroll=tiles,
            )
        for i in range(2 * pairs):
            sums[i] = totals[i]

    line = part[...]
    for i in range(2 * pairs):
        line = jnp.where(place == count + i, whole(sums[i]), line)
    part[...] = line

    def exchange(src, dst, target):
        return remote(src, dst, part_sem.at[0], part_sem.at[1], target)

    for target in range(n):

        @pl.when(me != target)
        def _():
            exchange(part, gathered.at[me], target).start()

    gathered[me] = line

    def close(chunk, carry):
        over_tiles(chunk, lambda t: update(steps - 1, odd, even, t, True))
        return carry

    if relayed > 1:
        lax.fori_loop(2 * relayed + 1, chunks, close, 0)
        after = upper * (relayed + 1)
        lax.fori_loop(after, relayed - 1 + upper * (relayed + 2), close, 0)
    if relayed:

        @pl.when(has_outer)
        def _():
            def arrive(chunk, carry):
                received_outer(odd, 1, late + chunk)
                return carry

            lax.fori_loop(0, relayed, arrive, 0)

    if relayed > 1:
        before = (1 - upper) * (relayed - 1)
        lax.fori_loop(before, 2 * relayed + 1 - upper * relayed, close, 0)
    else:
        lax.fori_loop(0, chunks, close, 0)
    if relayed:

        @pl.when(has_outer)
        def _():
            returned(0, relayed, 1).wait_send()

    sent(even, 0)
    sent(odd, 1)
    arriving = gathered.at[pl.ds(0, n - 1)]
    everything = exchange(arriving, arriving, inner_target)
    everything.wait_recv()
    line = gathered[0]
    for k in range(1, n):
        line = line + gathered[k]
    summed[...] = line
    everything.wait_send()


def publish(
    pairs,
    final,
    grad,
    pool,
    summed,
    final_hbm,
    grad_hbm,
    direction_hbm,
    direction,
    sem,
):
    rows, cols = grad.shape[1], grad.shape[2]
    copies = [
        pltpu.make_async_copy(final, final_hbm, sem.at[0]),
        pltpu.make_async_copy(grad, grad_hbm, sem.at[1]),
    ]
    for copy in copies:
        copy.start()

    place = lax.broadcasted_iota(jnp.int32, (1, 128), 1)
    products = product_pairs(pairs)
    count = len(products)
    where_of = {pair: k for k, pair in enumerate(products)}
    for i in range(2 * pairs):
        where_of[(i, 2 * pairs)] = count + i
    line = summed[...]
    cache = {}

    def inner(a, b):
        key = (min(a, b), max(a, b))
        if key not in cache:
            chosen = jnp.where(place == where_of[key], line, 0.0)
            cache[key] = jnp.sum(chosen, axis=1, keepdims=True)
        return cache[key]

    gradient_at = 2 * pairs
    curvature = [inner(i, pairs + i) for i in range(pairs)]
    alphas = [None] * pairs
    for i in reversed(range(pairs)):
        value = inner(i, gradient_at)
        for j in range(i + 1, pairs):
            value = value - alphas[j] * inner(i, pairs + j)
        alphas[i] = value / curvature[i]
    newest = 2 * pairs - 1
    gamma = curvature[pairs - 1] / inner(newest, newest)
    changes = [-gamma * alphas[i] for i in range(pairs)]
    steps_coef = [None] * pairs
    for i in range(pairs):
        value = gamma * inner(pairs + i, gradient_at)
        for j in range(pairs):
            value = value + changes[j] * inner(pairs + i, pairs + j)
        for j in range(i):
            value = value + steps_coef[j] * inner(j, pairs + i)
        steps_coef[i] = alphas[i] - value / curvature[i]

    def spread(value):
        return -jnp.broadcast_to(value, (8, cols))

    by_grad = spread(gamma)
    by_taken = [spread(value) for value in steps_coef]
    by_change = [spread(value) for value in changes]

    def combine(t, carry):
        for plane in range(2):
            at = (plane, tile(8 * t))
            value = by_grad * grad[at]
            for i in range(pairs):
                value = value + by_taken[i] * pool[(i,) + at]
                value = value + by_change[i] * pool[(pairs + i,) + at]
            direction[at] = value
        return carry

    tiles = rows // 8
    pieces = PIECES
    while tiles % pieces:
        pieces -= 1
    for piece in range(pieces):
        first, count = piece * (tiles // pieces), tiles // pieces
        lax.fori_loop(first, first + count, combine, 0, unroll=True)
        span = pl.ds(8 * first, 8 * count)
        copy = pltpu.make_async_copy(
            direction.at[:, span], direction_hbm.at[:, span], sem.at[2 + piece]
        )
        copy.start()
        copies.append(copy)
    for copy in copies:
        copy.wait()


def on_device(
    n,
    samples,
    field_now,
    field_before,
    lame_lambda,
    shear_modulus,
    density,
    source_field,
    wavelet,
    prior_mean,
    steps_taken,
    grad_change,
):
    comps, depth, rows, cols = field_now.shape
    pairs = steps_taken.shape[0]
    steps = wavelet.shape[0]
    size = chunk_rows(rows)
    chunks = rows // size
    relayed = 3 * chunks // 10
    assist = samples > comps and 8 <= n <= steps + 1 and steps >= 6 and chunks > 4
    helpers = comps - 1 if assist else 0
    f32 = jnp.float32
    state = pltpu.VMEM((comps, depth + 2, rows + 2 * PAD, cols), f32)
    model = pltpu.VMEM((depth, rows, cols), f32)
    returned = pltpu.VMEM((max(relayed, 1) * size, cols), f32)
    dma = pltpu.SemaphoreType.DMA
    anywhere = pl.BlockSpec(memory_space=pltpu.HBM)
    free = pl.BlockSpec(memory_space=pl.ANY)
    in_vmem = pl.BlockSpec(memory_space=pltpu.VMEM)
    results = pl.pallas_call(
        functools.partial(kernel, n, steps, pairs, size, relayed, helpers),
        out_shape=(
            pltpu.VMEM(field_now.shape, f32),
            pltpu.VMEM(lame_lambda.shape, f32),
            pltpu.VMEM((2 * pairs,) + lame_lambda.shape, f32),
            pltpu.VMEM((1, 128), f32),
        ),
        in_specs=[anywhere] * 10,
        out_specs=(in_vmem,) * 4,
        scratch_shapes=[
            state,
            state,
            pltpu.VMEM((4, depth, rows, cols), f32),
            pltpu.VMEM((comps, depth, rows, cols), f32),
            pltpu.SMEM((steps,), f32),
            pltpu.VMEM((2 * pairs, 8, 128), f32),
            pltpu.VMEM((1, 128), f32),
            pltpu.VMEM((n, 1, 128), f32),
            returned,
            returned,
            pltpu.VMEM((1, 2 * size, cols), f32),
            dma((2,)),
            dma((2,)),
            dma((2, chunks)),
            dma((3,)),
            dma((2,)),
            dma((1,)),
            pltpu.SemaphoreType.REGULAR,
        ],
        compiler_params=pltpu.CompilerParams(
            collective_id=0, has_side_effects=True, vmem_limit_bytes=63000000
        ),
    )(
        field_now,
        field_before,
        lame_lambda,
        shear_modulus,
        density,
        source_field,
        wavelet,
        prior_mean,
        steps_taken,
        grad_change,
    )
    return pl.pallas_call(
        functools.partial(publish, pairs),
        out_shape=tuple(
            jax.ShapeDtypeStruct(shape, f32)
            for shape in (field_now.shape, lame_lambda.shape, lame_lambda.shape)
        ),
        in_specs=[in_vmem] * 4,
        out_specs=(free, free, free),
        scratch_shapes=[model, dma((2 + PIECES,))],
        compiler_params=pltpu.CompilerParams(vmem_limit_bytes=4 * 1024 * 1024),
    )(*[pltpu.with_memory_space_constraint(value, pltpu.VMEM) for value in results])


def solution(mesh):
    n = mesh.shape["gz"]
    fields = P("sample", "gz", None, None)
    models = P("gz", "sample", None)
    placed = (
        fields,
        fields,
        models,
        models,
        models,
        fields,
        P("sample"),
        models,
        fields,
        fields,
    )
    return jax.shard_map(
        functools.partial(on_device, n, mesh.shape["sample"]),
        mesh=mesh,
        in_specs=placed,
        out_specs=(fields, models, models),
        check_vma=False,
    )
```

```python
import functools

import jax
import jax.numpy as jnp
from jax import lax
from jax.experimental import pallas as pl
from jax.experimental.pallas import tpu as pltpu
from jax.sharding import PartitionSpec as P

PAD = 8
CHUNK_ROWS = 16
PIECES = 4
RELAY_AT = 0


def chunk_rows(rows):
    size = CHUNK_ROWS
    while rows % size:
        size //= 2
    return size


def tile(start):
    return pl.ds(pl.multiple_of(start, 8), 8)


def fold(value):
    out = value[:, 0:128]
    for k in range(1, value.shape[1] // 128):
        out = out + value[:, 128 * k : 128 * (k + 1)]
    return out


def whole(value):
    return jnp.sum(jnp.sum(value, axis=0, keepdims=True), axis=1, keepdims=True)


def product_pairs(pairs):
    found = [(i, pairs + j) for i in range(pairs) for j in range(pairs)]
    return found + [(pairs + i, pairs + j) for i in range(pairs) for j in range(i, pairs)]


def kernel(
    n,
    steps,
    pairs,
    size,
    relayed,
    helpers,
    now_hbm,
    before_hbm,
    lame_hbm,
    shear_hbm,
    density_hbm,
    source_hbm,
    wavelet_hbm,
    prior_hbm,
    taken_hbm,
    change_hbm,
    final,
    grad,
    pool,
    summed,
    even,
    odd,
    models,
    source,
    wavelet,
    sums,
    part,
    gathered,
    product_out,
    product_in,
    detour,
    send_sem,
    inner_sem,
    outer_sem,
    product_sem,
    part_sem,
    detour_sem,
    ready,
):
    me = lax.axis_index("gz")
    rows, cols = grad.shape[1], grad.shape[2]
    chunks = rows // size
    tiles = size // 8
    upper = lax.rem(me, 2)
    has_outer = (me > 0) & (me < n - 1)
    inside = pl.ds(PAD, rows)
    chained = n - 1 <= steps
    inner_target = me + 1 - 2 * upper
    outer_target = lax.rem(me + n - 1 + 2 * upper, n)
    inner_plane, outer_plane = 2 - upper, 1 + upper
    inner_halo, outer_halo = 3 - 3 * upper, 3 * upper
    early = relayed * upper
    late = relayed - early
    lame, shear, coeff, prior = (models.at[i] for i in range(4))
    taken, change = pool.at[pl.ds(0, pairs)], pool.at[pl.ds(pairs, pairs)]

    sample = lax.axis_index("sample")
    below, above = n - 3, n - 2
    assisted = (sample == 0) & ((me == below) | (me == above))
    helping = (sample >= 1) & (sample <= helpers)
    carries = helping & ((me == below - 1) | (me == above + 1))
    stripped = chunks - 3
    strip = pl.ds(PAD + stripped * size, 3 * size)

    barrier = pltpu.get_barrier_semaphore()

    def greet(device):
        pl.semaphore_signal(
            barrier, inc=1, device_id={"gz": device}, device_id_type=pl.DeviceIdType.MESH
        )

    def greet_across(semaphore, target_sample, device):
        pl.semaphore_signal(
            semaphore,
            inc=1,
            device_id={"sample": target_sample, "gz": device},
            device_id_type=pl.DeviceIdType.MESH,
        )

    if chained:

        @pl.when(has_outer)
        def _():
            greet(outer_target)

        greet(inner_target)
        if helpers:

            @pl.when(assisted)
            def _():
                for helper in range(1, helpers + 1):
                    greet_across(barrier, helper, inner_target)

    else:
        for k in range(1, n):
            greet(lax.rem(me + k, n))

    loads = [
        pltpu.make_async_copy(src, dst, sem)
        for sem, src, dst in (
            (
                outer_sem.at[1, 0],
                now_hbm.at[:, :, pl.ds(0, size)],
                even.at[:, pl.ds(1, 2), pl.ds(PAD, size)],
            ),
            (
                inner_sem.at[1],
                now_hbm.at[:, :, pl.ds(size, rows - size)],
                even.at[:, pl.ds(1, 2), pl.ds(PAD + size, rows - size)],
            ),
            (product_sem.at[0], lame_hbm, lame),
            (product_sem.at[0], shear_hbm, shear),
            (product_sem.at[0], density_hbm, coeff),
            (product_sem.at[0], prior_hbm, prior),
            (product_sem.at[1], before_hbm, odd.at[:, pl.ds(1, 2), inside]),
            (part_sem.at[0], source_hbm, source),
            (send_sem.at[1], wavelet_hbm, wavelet),
            (part_sem.at[1], taken_hbm, taken),
            (part_sem.at[1], change_hbm, change),
        )
    ]
    for load in loads:
        load.start()

    def remote(src, dst, send, recv, target, target_sample=None):
        device = {"gz": target}
        if target_sample is not None:
            device["sample"] = target_sample
        return pltpu.make_async_remote_copy(
            src_ref=src,
            dst_ref=dst,
            send_sem=send,
            recv_sem=recv,
            device_id=device,
            device_id_type=pl.DeviceIdType.MESH,
        )

    def span(chunk):
        return pl.ds(pl.multiple_of(PAD + chunk * size, 8), size)

    def send_inner(ref, parity, chunk):
        remote(
            ref.at[:, inner_plane, span(chunk)],
            ref.at[:, 3 * upper, span(chunk)],
            send_sem.at[parity],
            inner_sem.at[parity],
            inner_target,
        ).start()

    def send_outer(ref, parity, chunk):
        remote(
            ref.at[:, outer_plane, span(chunk)],
            ref.at[:, 3 - 3 * upper, span(chunk)],
            send_sem.at[parity],
            outer_sem.at[parity, chunk],
            outer_target,
        ).start()

    def send_strips(ref, parity):
        for helper in range(1, helpers + 1):
            remote(
                ref.at[helper - 1, outer_plane, strip],
                detour.at[parity],
                send_sem.at[parity],
                detour_sem.at[parity],
                inner_target,
                helper,
            ).start()

    def pass_on(ref, parity):
        return remote(
            detour.at[parity],
            ref.at[sample - 1, 3 * upper, strip],
            part_sem.at[0],
            detour_sem.at[parity],
            me + 2 - 4 * upper,
            0,
        )

    def received_strips(ref, parity):
        strips = ref.at[pl.ds(0, helpers), outer_halo, strip]
        remote(strips, strips, send_sem.at[parity], detour_sem.at[parity], outer_target).wait_recv()

    def send(ref, parity, chunk):
        @pl.when(has_outer)
        def _():
            send_outer(ref, parity, chunk)

        send_inner(ref, parity, chunk)

    others = pl.ds(helpers, even.shape[0] - helpers)

    def send_but_strips(ref, parity, chunk):
        cut = assisted & (chunk >= stripped)

        @pl.when(has_outer & jnp.logical_not(cut))
        def _():
            send_outer(ref, parity, chunk)

        @pl.when(cut)
        def _():
            remote(
                ref.at[others, outer_plane, span(chunk)],
                ref.at[others, 3 - 3 * upper, span(chunk)],
                send_sem.at[parity],
                outer_sem.at[parity, chunk],
                outer_target,
            ).start()

        send_inner(ref, parity, chunk)

    def sent(ref, parity):
        def wait(planes):
            whole_planes = ref.at[:, planes, inside]
            remote(
                whole_planes, whole_planes, send_sem.at[parity], inner_sem.at[parity], inner_target
            ).wait_send()

        @pl.when(has_outer)
        def _():
            wait(pl.ds(1, 2))

        @pl.when(jnp.logical_not(has_outer))
        def _():
            wait(pl.ds(1, 1))

    def received_inner(ref, parity):
        halo = ref.at[:, inner_halo, inside]
        remote(halo, halo, send_sem.at[parity], inner_sem.at[parity], inner_target).wait_recv()

    def received_outer(ref, parity, chunk):
        halo = ref.at[:, outer_halo, span(chunk)]
        remote(
            halo, halo, send_sem.at[parity], outer_sem.at[parity, chunk], outer_target
        ).wait_recv()

    if chained:
        expected = 1 + has_outer.astype(jnp.int32)
        if helpers:
            expected = expected + carries.astype(jnp.int32)
        pl.semaphore_wait(barrier, expected)
    else:
        pl.semaphore_wait(barrier, n - 1)

    if helpers:

        @pl.when(carries)
        def _():
            greet_across(ready, 0, me + 1 - 2 * upper)

    loads[0].wait()
    send(even, 0, 0)
    loads[1].wait()

    def first(chunk, carry):
        (send_but_strips if helpers else send)(even, 0, chunk)
        return carry

    lax.fori_loop(1, chunks, first, 0)

    edge = jnp.zeros((even.shape[0], 4, PAD, cols), jnp.float32)
    for ref in (even, odd):
        ref[:, :, pl.ds(0, PAD)] = edge
        ref[:, :, pl.ds(PAD + rows, PAD)] = edge

    @pl.when(jnp.logical_not(has_outer))
    def _():
        def body(t, carry):
            for ref in (even, odd):
                for comp in range(3):
                    ref[comp, outer_halo, tile(PAD + 8 * t)] = jnp.zeros((8, cols), jnp.float32)
            return carry

        lax.fori_loop(0, rows // 8, body, 0)

    if helpers:

        @pl.when(assisted)
        def _():
            pl.semaphore_wait(ready, helpers)
            send_strips(even, 0)

    pltpu.make_async_copy(models, models, product_sem.at[0]).wait()

    def prepare(t, carry):
        for plane in range(2):
            at = (plane, tile(8 * t))
            lame[at] = lame[at] + shear[at]
            coeff[at] = 0.04 / coeff[at]
            grad[at] = jnp.zeros((8, cols), jnp.float32)
        return carry

    lax.fori_loop(0, rows // 8, prepare, 0)
    for load in loads[6:9]:
        load.wait()
    pltpu.make_async_copy(pool, pool, part_sem.at[1]).wait()

    products = product_pairs(pairs)
    count = len(products)

    def stored(t, totals):
        totals = list(totals)
        for plane in range(2):
            vectors = [pool[i, plane, tile(8 * t)] for i in range(2 * pairs)]
            for k, (a, b) in enumerate(products):
                totals[k] = totals[k] + fold(vectors[a] * vectors[b])
        return tuple(totals)

    totals = lax.fori_loop(
        0, rows // 8, stored, tuple(jnp.zeros((8, 128), jnp.float32) for _ in products)
    )
    place = lax.broadcasted_iota(jnp.int32, (1, 128), 1)

    line = jnp.zeros((1, 128), jnp.float32)
    for k in range(count):
        line = jnp.where(place == k, whole(totals[k]), line)
    part[...] = line

    row_at = lax.broadcasted_iota(jnp.int32, (8, cols), 0)
    col_at = lax.broadcasted_iota(jnp.int32, (8, cols), 1)
    is_top, is_bottom = row_at == 0, row_at == 7
    is_left, is_right = col_at == 0, col_at == cols - 1

    def along_x(previous, value, following):
        minus = pltpu.roll(jnp.where(is_bottom, previous, value), 1, 0)
        plus = pltpu.roll(jnp.where(is_top, following, value), 7, 0)
        return minus, plus

    def along_y(value):
        minus = jnp.where(is_left, 0.0, pltpu.roll(value, 1, 1))
        plus = jnp.where(is_right, 0.0, pltpu.roll(value, cols - 1, 1))
        return minus, plus

    def delta_y(value):
        minus, plus = along_y(value)
        return plus - minus

    def update(step, current, other, t, last=False):
        amplitude = wavelet[step]

        def load(comp, plane, shift=0):
            return current[comp, plane, tile(PAD + 8 * (t + shift))]

        for plane in range(2):
            low, mid, high = plane, plane + 1, plane + 2
            at = tile(8 * t)
            here = tile(PAD + 8 * t)

            def delta_z(comp, shift=0):
                return load(comp, high, shift) - load(comp, low, shift)

            def delta_xz(comp, centre):
                minus, plus = along_x(delta_z(comp, -1), centre, delta_z(comp, 1))
                return plus - minus

            centre = [load(comp, mid) for comp in range(3)]
            diff = [delta_z(comp) for comp in range(3)]
            total = [load(comp, high) + load(comp, low) for comp in range(3)]
            xs = [along_x(load(comp, mid, -1), centre[comp], load(comp, mid, 1)) for comp in range(3)]
            ys = [along_y(centre[comp]) for comp in range(3)]
            sum_x = [minus + plus for minus, plus in xs]
            sum_y = [minus + plus for minus, plus in ys]
            dx = [plus - minus for minus, plus in xs]
            lap = [
                (total[comp] + sum_x[comp]) + (sum_y[comp] - 6.0 * centre[comp])
                for comp in range(3)
            ]
            mixed = [
                delta_xz(1, diff[1]) + delta_y(diff[2]),
                delta_xz(0, diff[0]) + delta_y(dx[2]),
                delta_y(diff[0] + dx[1]),
            ]
            own = [total[0], sum_x[1], sum_y[2]]
            both = lame[plane, at]
            mu = shear[plane, at]
            rate = coeff[plane, at]
            if not last:
                grad[plane, at] = grad[plane, at] + (
                    centre[0] * lap[0] + centre[1] * lap[1] + centre[2] * lap[2]
                )
            for comp in range(3):
                doubled = 2.0 * centre[comp]
                elastic = both * ((own[comp] - doubled) + 0.25 * mixed[comp]) + mu * lap[comp]
                value = (
                    doubled
                    - other[comp, mid, here]
                    + rate * (elastic + amplitude * source[comp, plane, at])
                )
                if last:
                    final[comp, plane, at] = value
                else:
                    other[comp, mid, here] = value

    def over_tiles(chunk, body):
        def tile_body(t, carry):
            body(chunk * tiles + t)
            return carry

        lax.fori_loop(0, tiles, tile_body, 0)

    def wait_outer(ref, parity, chunk):
        @pl.when(has_outer)
        def _():
            received_outer(ref, parity, chunk)

    def wait_all_but_strips(ref, parity, chunk):
        @pl.when(assisted & (chunk == stripped))
        def _():
            received_strips(ref, parity)

        @pl.when(has_outer & jnp.logical_not(assisted & (chunk >= stripped)))
        def _():
            received_outer(ref, parity, chunk)

        @pl.when(assisted & (chunk >= stripped))
        def _():
            rest = ref.at[others, outer_halo, span(chunk)]
            remote(
                rest, rest, send_sem.at[parity], outer_sem.at[parity, chunk], outer_target
            ).wait_recv()

    def advance(step, current, other, parity, relay, detours=False):
        @pl.when(step > 0)
        def _():
            sent(other, 1 - parity)

        received_inner(current, parity)
        wait_outer(current, parity, 0)

        def chunk_body(chunk, carry):
            @pl.when(chunk + 1 < chunks)
            def _():
                (wait_all_but_strips if detours else wait_outer)(current, parity, chunk + 1)

            if detours:

                @pl.when(carries & (chunk == RELAY_AT))
                def _():
                    received = detour.at[parity]
                    remote(
                        received, received, part_sem.at[0], detour_sem.at[parity], inner_target
                    ).wait_recv()
                    pass_on(current, parity).start()

            over_tiles(chunk, lambda t: update(step, current, other, t))
            if relay:

                @pl.when(has_outer & ((chunk < early) | (chunk >= early + relayed)))
                def _():
                    send_outer(other, 1 - parity, chunk)

                send_inner(other, 1 - parity, chunk)
            else:
                send(other, 1 - parity, chunk)
            return carry

        lax.fori_loop(0, chunks, chunk_body, 0)

    def two_steps(k, carry):
        advance(2 * k, even, odd, 0, False)
        advance(2 * k + 1, odd, even, 1, False)
        return carry

    if helpers:
        advance(0, even, odd, 0, False, True)

        @pl.when(carries)
        def _():
            pass_on(even, 0).wait_send()

        advance(1, odd, even, 1, False)

    lax.fori_loop(1 if helpers else 0, steps // 2 - 1, two_steps, 0)
    advance(steps - 2, even, odd, 0, True)

    def across(t):
        here = tile(PAD + 8 * t)
        value = odd[0, outer_plane, here] * odd[0, outer_halo, here]
        for comp in range(1, 3):
            value = value + odd[comp, outer_plane, here] * odd[comp, outer_halo, here]
        return value

    def returned(first, number, sem):
        where = pl.ds(first * size, number * size)
        return remote(
            product_out.at[where],
            product_in.at[where],
            product_sem.at[0],
            product_sem.at[sem],
            outer_target,
        )

    pieces = [(0, relayed - 1, 1), (relayed - 1, 1, 2)] if relayed > 1 else [(0, relayed, 1)]
    pieces = [piece for piece in pieces if piece[1]]
    if pieces:

        @pl.when(has_outer)
        def _():
            def multiply(chunk, carry):
                received_outer(odd, 1, early + chunk)
                for k in range(tiles):
                    t = chunk * tiles + k
                    product_out[tile(8 * t)] = across(early * tiles + t)
                return carry

            for piece in pieces:
                lax.fori_loop(piece[0], piece[0] + piece[1], multiply, 0)
                returned(*piece).start()

            def follow(chunk, carry):
                send_outer(odd, 1, early + chunk)
                return carry

            lax.fori_loop(0, relayed, follow, 0)

    received_inner(odd, 1)

    def weigh(totals, at, value):
        return tuple(
            totals[i] + fold(pool[(i,) + at] * value) for i in range(2 * pairs)
        )

    def own_part(t, totals):
        def load(comp, plane, shift=0):
            return odd[comp, plane, tile(PAD + 8 * (t + shift))]

        for mid, around in ((inner_plane, (outer_plane, inner_halo)), (outer_plane, (inner_plane,))):
            at = (mid - 1, tile(8 * t))
            value = None
            for comp in range(3):
                centre = load(comp, mid)
                minus_x, plus_x = along_x(load(comp, mid, -1), centre, load(comp, mid, 1))
                minus_y, plus_y = along_y(centre)
                total = load(comp, around[0])
                for plane in around[1:]:
                    total = total + load(comp, plane)
                lap = (total + (minus_x + plus_x)) + ((minus_y + plus_y) - 6.0 * centre)
                value = centre * lap if value is None else value + centre * lap
            value = (shear[at] - prior[at]) + 0.02 * (grad[at] + value)
            grad[at] = value
            totals = weigh(totals, at, value)
        return totals

    totals = lax.fori_loop(
        0,
        rows // 8,
        own_part,
        tuple(jnp.zeros((8, 128), jnp.float32) for _ in range(2 * pairs)),
        unroll=2,
    )
    for i in range(2 * pairs):
        sums[i] = totals[i]

    @pl.when(has_outer)
    def _():
        def add(t, product, totals):
            at = (outer_plane - 1, tile(8 * t))
            value = 0.02 * product
            grad[at] = grad[at] + value
            return weigh(totals, at, value)

        def added(products, start):
            return lambda t, totals: add(start * tiles + t, products[tile(8 * t)], totals)

        totals = tuple(sums[i] for i in range(2 * pairs))
        if relayed:
            totals = lax.fori_loop(0, relayed * tiles, added(product_out, early), totals)

        def direct(chunk, totals):
            received_outer(odd, 1, chunk)
            for k in range(tiles):
                t = chunk * tiles + k
                totals = add(t, across(t), totals)
            return totals

        totals = lax.fori_loop(2 * relayed, chunks, direct, totals)
        for piece in pieces:
            returned(*piece).wait_recv()
            totals = lax.fori_loop(
                piece[0] * tiles,
                (piece[0] + piece[1]) * tiles,
                added(product_in, late),
                totals,
                unroll=tiles,
            )
        for i in range(2 * pairs):
            sums[i] = totals[i]

    line = part[...]
    for i in range(2 * pairs):
        line = jnp.where(place == count + i, whole(sums[i]), line)
    part[...] = line

    def exchange(src, dst, target):
        return remote(src, dst, part_sem.at[0], part_sem.at[1], target)

    for target in range(n):

        @pl.when(me != target)
        def _():
            exchange(part, gathered.at[me], target).start()

    gathered[me] = line

    def close(chunk, carry):
        over_tiles(chunk, lambda t: update(steps - 1, odd, even, t, True))
        return carry

    if relayed > 1:
        lax.fori_loop(2 * relayed + 1, chunks, close, 0)
        after = upper * (relayed + 1)
        lax.fori_loop(after, relayed - 1 + upper * (relayed + 2), close, 0)
    if relayed:

        @pl.when(has_outer)
        def _():
            def arrive(chunk, carry):
                received_outer(odd, 1, late + chunk)
                return carry

            lax.fori_loop(0, relayed, arrive, 0)

    if relayed > 1:
        before = (1 - upper) * (relayed - 1)
        lax.fori_loop(before, 2 * relayed + 1 - upper * relayed, close, 0)
    else:
        lax.fori_loop(0, chunks, close, 0)
    if relayed:

        @pl.when(has_outer)
        def _():
            returned(0, relayed, 1).wait_send()

    sent(even, 0)
    sent(odd, 1)
    arriving = gathered.at[pl.ds(0, n - 1)]
    everything = exchange(arriving, arriving, inner_target)
    everything.wait_recv()
    line = gathered[0]
    for k in range(1, n):
        line = line + gathered[k]
    summed[...] = line
    everything.wait_send()


def publish(
    pairs,
    final,
    grad,
    pool,
    summed,
    final_hbm,
    grad_hbm,
    direction_hbm,
    direction,
    sem,
):
    rows, cols = grad.shape[1], grad.shape[2]
    copies = [
        pltpu.make_async_copy(final, final_hbm, sem.at[0]),
        pltpu.make_async_copy(grad, grad_hbm, sem.at[1]),
    ]
    for copy in copies:
        copy.start()

    place = lax.broadcasted_iota(jnp.int32, (1, 128), 1)
    products = product_pairs(pairs)
    count = len(products)
    where_of = {pair: k for k, pair in enumerate(products)}
    for i in range(2 * pairs):
        where_of[(i, 2 * pairs)] = count + i
    line = summed[...]
    cache = {}

    def inner(a, b):
        key = (min(a, b), max(a, b))
        if key not in cache:
            chosen = jnp.where(place == where_of[key], line, 0.0)
            cache[key] = jnp.sum(chosen, axis=1, keepdims=True)
        return cache[key]

    gradient_at = 2 * pairs
    curvature = [inner(i, pairs + i) for i in range(pairs)]
    alphas = [None] * pairs
    for i in reversed(range(pairs)):
        value = inner(i, gradient_at)
        for j in range(i + 1, pairs):
            value = value - alphas[j] * inner(i, pairs + j)
        alphas[i] = value / curvature[i]
    newest = 2 * pairs - 1
    gamma = curvature[pairs - 1] / inner(newest, newest)
    changes = [-gamma * alphas[i] for i in range(pairs)]
    steps_coef = [None] * pairs
    for i in range(pairs):
        value = gamma * inner(pairs + i, gradient_at)
        for j in range(pairs):
            value = value + changes[j] * inner(pairs + i, pairs + j)
        for j in range(i):
            value = value + steps_coef[j] * inner(j, pairs + i)
        steps_coef[i] = alphas[i] - value / curvature[i]

    def spread(value):
        return -jnp.broadcast_to(value, (8, cols))

    by_grad = spread(gamma)
    by_taken = [spread(value) for value in steps_coef]
    by_change = [spread(value) for value in changes]

    def combine(t, carry):
        for plane in range(2):
            at = (plane, tile(8 * t))
            value = by_grad * grad[at]
            for i in range(pairs):
                value = value + by_taken[i] * pool[(i,) + at]
                value = value + by_change[i] * pool[(pairs + i,) + at]
            direction[at] = value
        return carry

    tiles = rows // 8
    pieces = PIECES
    while tiles % pieces:
        pieces -= 1
    for piece in range(pieces):
        first, count = piece * (tiles // pieces), tiles // pieces
        lax.fori_loop(first, first + count, combine, 0, unroll=True)
        span = pl.ds(8 * first, 8 * count)
        copy = pltpu.make_async_copy(
            direction.at[:, span], direction_hbm.at[:, span], sem.at[2 + piece]
        )
        copy.start()
        copies.append(copy)
    for copy in copies:
        copy.wait()


def on_device(
    n,
    samples,
    field_now,
    field_before,
    lame_lambda,
    shear_modulus,
    density,
    source_field,
    wavelet,
    prior_mean,
    steps_taken,
    grad_change,
):
    comps, depth, rows, cols = field_now.shape
    pairs = steps_taken.shape[0]
    steps = wavelet.shape[0]
    size = chunk_rows(rows)
    chunks = rows // size
    relayed = 3 * chunks // 10
    assist = samples > comps and 8 <= n <= steps + 1 and steps >= 6 and chunks > 4
    helpers = comps - 1 if assist else 0
    f32 = jnp.float32
    state = pltpu.VMEM((comps, depth + 2, rows + 2 * PAD, cols), f32)
    model = pltpu.VMEM((depth, rows, cols), f32)
    returned = pltpu.VMEM((max(relayed, 1) * size, cols), f32)
    dma = pltpu.SemaphoreType.DMA
    anywhere = pl.BlockSpec(memory_space=pltpu.HBM)
    free = pl.BlockSpec(memory_space=pl.ANY)
    in_vmem = pl.BlockSpec(memory_space=pltpu.VMEM)
    results = pl.pallas_call(
        functools.partial(kernel, n, steps, pairs, size, relayed, helpers),
        out_shape=(
            pltpu.VMEM(field_now.shape, f32),
            pltpu.VMEM(lame_lambda.shape, f32),
            pltpu.VMEM((2 * pairs,) + lame_lambda.shape, f32),
            pltpu.VMEM((1, 128), f32),
        ),
        in_specs=[anywhere] * 10,
        out_specs=(in_vmem,) * 4,
        scratch_shapes=[
            state,
            state,
            pltpu.VMEM((4, depth, rows, cols), f32),
            pltpu.VMEM((comps, depth, rows, cols), f32),
            pltpu.SMEM((steps,), f32),
            pltpu.VMEM((2 * pairs, 8, 128), f32),
            pltpu.VMEM((1, 128), f32),
            pltpu.VMEM((n, 1, 128), f32),
            returned,
            returned,
            pltpu.VMEM((1, 3 * size, cols), f32),
            dma((2,)),
            dma((2,)),
            dma((2, chunks)),
            dma((3,)),
            dma((2,)),
            dma((1,)),
            pltpu.SemaphoreType.REGULAR,
        ],
        compiler_params=pltpu.CompilerParams(
            collective_id=0, has_side_effects=True, vmem_limit_bytes=63000000
        ),
    )(
        field_now,
        field_before,
        lame_lambda,
        shear_modulus,
        density,
        source_field,
        wavelet,
        prior_mean,
        steps_taken,
        grad_change,
    )
    return pl.pallas_call(
        functools.partial(publish, pairs),
        out_shape=tuple(
            jax.ShapeDtypeStruct(shape, f32)
            for shape in (field_now.shape, lame_lambda.shape, lame_lambda.shape)
        ),
        in_specs=[in_vmem] * 4,
        out_specs=(free, free, free),
        scratch_shapes=[model, dma((2 + PIECES,))],
        compiler_params=pltpu.CompilerParams(vmem_limit_bytes=4 * 1024 * 1024),
    )(*[pltpu.with_memory_space_constraint(value, pltpu.VMEM) for value in results])


def solution(mesh):
    n = mesh.shape["gz"]
    fields = P("sample", "gz", None, None)
    models = P("gz", "sample", None)
    placed = (
        fields,
        fields,
        models,
        models,
        models,
        fields,
        P("sample"),
        models,
        fields,
        fields,
    )
    return jax.shard_map(
        functools.partial(on_device, n, mesh.shape["sample"]),
        mesh=mesh,
        in_specs=placed,
        out_specs=(fields, models, models),
        check_vma=False,
    )
```

```python
import functools

import jax
import jax.numpy as jnp
from jax import lax
from jax.experimental import pallas as pl
from jax.experimental.pallas import tpu as pltpu
from jax.sharding import PartitionSpec as P

PAD = 8
CHUNK_ROWS = 16
PIECES = 4
RELAY_AT = 0


def chunk_rows(rows):
    size = CHUNK_ROWS
    while rows % size:
        size //= 2
    return size


def tile(start):
    return pl.ds(pl.multiple_of(start, 8), 8)


def fold(value):
    out = value[:, 0:128]
    for k in range(1, value.shape[1] // 128):
        out = out + value[:, 128 * k : 128 * (k + 1)]
    return out


def whole(value):
    return jnp.sum(jnp.sum(value, axis=0, keepdims=True), axis=1, keepdims=True)


def product_pairs(pairs):
    found = [(i, pairs + j) for i in range(pairs) for j in range(pairs)]
    return found + [(pairs + i, pairs + j) for i in range(pairs) for j in range(i, pairs)]


def kernel(
    n,
    steps,
    pairs,
    size,
    relayed,
    helpers,
    now_hbm,
    before_hbm,
    lame_hbm,
    shear_hbm,
    density_hbm,
    source_hbm,
    wavelet_hbm,
    prior_hbm,
    taken_hbm,
    change_hbm,
    final,
    grad,
    pool,
    summed,
    even,
    odd,
    models,
    source,
    wavelet,
    sums,
    part,
    gathered,
    product_out,
    product_in,
    detour,
    send_sem,
    inner_sem,
    outer_sem,
    product_sem,
    part_sem,
    detour_sem,
    ready,
):
    me = lax.axis_index("gz")
    rows, cols = grad.shape[1], grad.shape[2]
    chunks = rows // size
    tiles = size // 8
    upper = lax.rem(me, 2)
    has_outer = (me > 0) & (me < n - 1)
    inside = pl.ds(PAD, rows)
    chained = n - 1 <= steps
    inner_target = me + 1 - 2 * upper
    outer_target = lax.rem(me + n - 1 + 2 * upper, n)
    inner_plane, outer_plane = 2 - upper, 1 + upper
    inner_halo, outer_halo = 3 - 3 * upper, 3 * upper
    early = relayed * upper
    late = relayed - early
    lame, shear, coeff, prior = (models.at[i] for i in range(4))
    taken, change = pool.at[pl.ds(0, pairs)], pool.at[pl.ds(pairs, pairs)]

    sample = lax.axis_index("sample")
    below, above = n - 3, n - 2
    assisted = (sample == 0) & ((me == below) | (me == above))
    helping = (sample >= 1) & (sample <= helpers)
    carries = helping & ((me == below - 1) | (me == above + 1))
    stripped = chunks - 2
    strip = pl.ds(PAD + stripped * size, 2 * size)

    barrier = pltpu.get_barrier_semaphore()

    def greet(device):
        pl.semaphore_signal(
            barrier, inc=1, device_id={"gz": device}, device_id_type=pl.DeviceIdType.MESH
        )

    def greet_across(semaphore, target_sample, device):
        pl.semaphore_signal(
            semaphore,
            inc=1,
            device_id={"sample": target_sample, "gz": device},
            device_id_type=pl.DeviceIdType.MESH,
        )

    if chained:

        @pl.when(has_outer)
        def _():
            greet(outer_target)

        greet(inner_target)
        if helpers:

            @pl.when(assisted)
            def _():
                for helper in range(1, helpers + 1):
                    greet_across(barrier, helper, inner_target)

    else:
        for k in range(1, n):
            greet(lax.rem(me + k, n))

    loads = [
        pltpu.make_async_copy(src, dst, sem)
        for sem, src, dst in (
            (
                outer_sem.at[1, 0],
                now_hbm.at[:, :, pl.ds(0, size)],
                even.at[:, pl.ds(1, 2), pl.ds(PAD, size)],
            ),
            (
                inner_sem.at[1],
                now_hbm.at[:, :, pl.ds(size, rows - size)],
                even.at[:, pl.ds(1, 2), pl.ds(PAD + size, rows - size)],
            ),
            (product_sem.at[0], lame_hbm, lame),
            (product_sem.at[0], shear_hbm, shear),
            (product_sem.at[0], density_hbm, coeff),
            (product_sem.at[0], prior_hbm, prior),
            (product_sem.at[1], before_hbm, odd.at[:, pl.ds(1, 2), inside]),
            (part_sem.at[0], source_hbm, source),
            (send_sem.at[1], wavelet_hbm, wavelet),
            (part_sem.at[1], taken_hbm, taken),
            (part_sem.at[1], change_hbm, change),
        )
    ]
    for load in loads:
        load.start()

    def remote(src, dst, send, recv, target, target_sample=None):
        device = {"gz": target}
        if target_sample is not None:
            device["sample"] = target_sample
        return pltpu.make_async_remote_copy(
            src_ref=src,
            dst_ref=dst,
            send_sem=send,
            recv_sem=recv,
            device_id=device,
            device_id_type=pl.DeviceIdType.MESH,
        )

    def span(chunk):
        return pl.ds(pl.multiple_of(PAD + chunk * size, 8), size)

    def send_inner(ref, parity, chunk):
        remote(
            ref.at[:, inner_plane, span(chunk)],
            ref.at[:, 3 * upper, span(chunk)],
            send_sem.at[parity],
            inner_sem.at[parity],
            inner_target,
        ).start()

    def send_outer(ref, parity, chunk):
        remote(
            ref.at[:, outer_plane, span(chunk)],
            ref.at[:, 3 - 3 * upper, span(chunk)],
            send_sem.at[parity],
            outer_sem.at[parity, chunk],
            outer_target,
        ).start()

    def send_strips(ref, parity):
        for helper in range(1, helpers + 1):
            remote(
                ref.at[helper - 1, outer_plane, strip],
                detour.at[parity],
                send_sem.at[parity],
                detour_sem.at[parity],
                inner_target,
                helper,
            ).start()

    def pass_on(ref, parity):
        return remote(
            detour.at[parity],
            ref.at[sample - 1, 3 * upper, strip],
            part_sem.at[0],
            detour_sem.at[parity],
            me + 2 - 4 * upper,
            0,
        )

    def received_strips(ref, parity):
        strips = ref.at[pl.ds(0, helpers), outer_halo, strip]
        remote(strips, strips, send_sem.at[parity], detour_sem.at[parity], outer_target).wait_recv()

    def send(ref, parity, chunk):
        @pl.when(has_outer)
        def _():
            send_outer(ref, parity, chunk)

        send_inner(ref, parity, chunk)

    others = pl.ds(helpers, even.shape[0] - helpers)

    def send_but_strips(ref, parity, chunk):
        cut = assisted & (chunk >= stripped)

        @pl.when(has_outer & jnp.logical_not(cut))
        def _():
            send_outer(ref, parity, chunk)

        @pl.when(cut)
        def _():
            remote(
                ref.at[others, outer_plane, span(chunk)],
                ref.at[others, 3 - 3 * upper, span(chunk)],
                send_sem.at[parity],
                outer_sem.at[parity, chunk],
                outer_target,
            ).start()

        send_inner(ref, parity, chunk)

    def sent(ref, parity):
        def wait(planes):
            whole_planes = ref.at[:, planes, inside]
            remote(
                whole_planes, whole_planes, send_sem.at[parity], inner_sem.at[parity], inner_target
            ).wait_send()

        @pl.when(has_outer)
        def _():
            wait(pl.ds(1, 2))

        @pl.when(jnp.logical_not(has_outer))
        def _():
            wait(pl.ds(1, 1))

    def received_inner(ref, parity):
        halo = ref.at[:, inner_halo, inside]
        remote(halo, halo, send_sem.at[parity], inner_sem.at[parity], inner_target).wait_recv()

    def received_outer(ref, parity, chunk):
        halo = ref.at[:, outer_halo, span(chunk)]
        remote(
            halo, halo, send_sem.at[parity], outer_sem.at[parity, chunk], outer_target
        ).wait_recv()

    if chained:
        expected = 1 + has_outer.astype(jnp.int32)
        if helpers:
            expected = expected + carries.astype(jnp.int32)
        pl.semaphore_wait(barrier, expected)
    else:
        pl.semaphore_wait(barrier, n - 1)

    if helpers:

        @pl.when(carries)
        def _():
            greet_across(ready, 0, me + 1 - 2 * upper)

    loads[0].wait()
    send(even, 0, 0)
    loads[1].wait()

    def first(chunk, carry):
        (send_but_strips if helpers else send)(even, 0, chunk)
        return carry

    lax.fori_loop(1, chunks, first, 0)

    if helpers:

        @pl.when(assisted)
        def _():
            pl.semaphore_wait(ready, helpers)
            send_strips(even, 0)

    edge = jnp.zeros((even.shape[0], 4, PAD, cols), jnp.float32)
    for ref in (even, odd):
        ref[:, :, pl.ds(0, PAD)] = edge
        ref[:, :, pl.ds(PAD + rows, PAD)] = edge

    @pl.when(jnp.logical_not(has_outer))
    def _():
        def body(t, carry):
            for ref in (even, odd):
                for comp in range(3):
                    ref[comp, outer_halo, tile(PAD + 8 * t)] = jnp.zeros((8, cols), jnp.float32)
            return carry

        lax.fori_loop(0, rows // 8, body, 0)

    pltpu.make_async_copy(models, models, product_sem.at[0]).wait()

    def prepare(t, carry):
        for plane in range(2):
            at = (plane, tile(8 * t))
            lame[at] = lame[at] + shear[at]
            coeff[at] = 0.04 / coeff[at]
            grad[at] = jnp.zeros((8, cols), jnp.float32)
        return carry

    lax.fori_loop(0, rows // 8, prepare, 0)
    for load in loads[6:9]:
        load.wait()
    pltpu.make_async_copy(pool, pool, part_sem.at[1]).wait()

    products = product_pairs(pairs)
    count = len(products)

    def stored(t, totals):
        totals = list(totals)
        for plane in range(2):
            vectors = [pool[i, plane, tile(8 * t)] for i in range(2 * pairs)]
            for k, (a, b) in enumerate(products):
                totals[k] = totals[k] + fold(vectors[a] * vectors[b])
        return tuple(totals)

    totals = lax.fori_loop(
        0, rows // 8, stored, tuple(jnp.zeros((8, 128), jnp.float32) for _ in products)
    )
    place = lax.broadcasted_iota(jnp.int32, (1, 128), 1)

    line = jnp.zeros((1, 128), jnp.float32)
    for k in range(count):
        line = jnp.where(place == k, whole(totals[k]), line)
    part[...] = line

    row_at = lax.broadcasted_iota(jnp.int32, (8, cols), 0)
    col_at = lax.broadcasted_iota(jnp.int32, (8, cols), 1)
    is_top, is_bottom = row_at == 0, row_at == 7
    is_left, is_right = col_at == 0, col_at == cols - 1

    def along_x(previous, value, following):
        minus = pltpu.roll(jnp.where(is_bottom, previous, value), 1, 0)
        plus = pltpu.roll(jnp.where(is_top, following, value), 7, 0)
        return minus, plus

    def along_y(value):
        minus = jnp.where(is_left, 0.0, pltpu.roll(value, 1, 1))
        plus = jnp.where(is_right, 0.0, pltpu.roll(value, cols - 1, 1))
        return minus, plus

    def delta_y(value):
        minus, plus = along_y(value)
        return plus - minus

    def update(step, current, other, t, last=False):
        amplitude = wavelet[step]

        def load(comp, plane, shift=0):
            return current[comp, plane, tile(PAD + 8 * (t + shift))]

        for plane in range(2):
            low, mid, high = plane, plane + 1, plane + 2
            at = tile(8 * t)
            here = tile(PAD + 8 * t)

            def delta_z(comp, shift=0):
                return load(comp, high, shift) - load(comp, low, shift)

            def delta_xz(comp, centre):
                minus, plus = along_x(delta_z(comp, -1), centre, delta_z(comp, 1))
                return plus - minus

            centre = [load(comp, mid) for comp in range(3)]
            diff = [delta_z(comp) for comp in range(3)]
            total = [load(comp, high) + load(comp, low) for comp in range(3)]
            xs = [along_x(load(comp, mid, -1), centre[comp], load(comp, mid, 1)) for comp in range(3)]
            ys = [along_y(centre[comp]) for comp in range(3)]
            sum_x = [minus + plus for minus, plus in xs]
            sum_y = [minus + plus for minus, plus in ys]
            dx = [plus - minus for minus, plus in xs]
            lap = [
                (total[comp] + sum_x[comp]) + (sum_y[comp] - 6.0 * centre[comp])
                for comp in range(3)
            ]
            mixed = [
                delta_xz(1, diff[1]) + delta_y(diff[2]),
                delta_xz(0, diff[0]) + delta_y(dx[2]),
                delta_y(diff[0] + dx[1]),
            ]
            own = [total[0], sum_x[1], sum_y[2]]
            both = lame[plane, at]
            mu = shear[plane, at]
            rate = coeff[plane, at]
            if not last:
                grad[plane, at] = grad[plane, at] + (
                    centre[0] * lap[0] + centre[1] * lap[1] + centre[2] * lap[2]
                )
            for comp in range(3):
                doubled = 2.0 * centre[comp]
                elastic = both * ((own[comp] - doubled) + 0.25 * mixed[comp]) + mu * lap[comp]
                value = (
                    doubled
                    - other[comp, mid, here]
                    + rate * (elastic + amplitude * source[comp, plane, at])
                )
                if last:
                    final[comp, plane, at] = value
                else:
                    other[comp, mid, here] = value

    def over_tiles(chunk, body):
        def tile_body(t, carry):
            body(chunk * tiles + t)
            return carry

        lax.fori_loop(0, tiles, tile_body, 0)

    def wait_outer(ref, parity, chunk):
        @pl.when(has_outer)
        def _():
            received_outer(ref, parity, chunk)

    def wait_all_but_strips(ref, parity, chunk):
        @pl.when(assisted & (chunk == stripped))
        def _():
            received_strips(ref, parity)

        @pl.when(has_outer & jnp.logical_not(assisted & (chunk >= stripped)))
        def _():
            received_outer(ref, parity, chunk)

        @pl.when(assisted & (chunk >= stripped))
        def _():
            rest = ref.at[others, outer_halo, span(chunk)]
            remote(
                rest, rest, send_sem.at[parity], outer_sem.at[parity, chunk], outer_target
            ).wait_recv()

    def advance(step, current, other, parity, relay, detours=False):
        @pl.when(step > 0)
        def _():
            sent(other, 1 - parity)

        received_inner(current, parity)
        wait_outer(current, parity, 0)

        def chunk_body(chunk, carry):
            @pl.when(chunk + 1 < chunks)
            def _():
                (wait_all_but_strips if detours else wait_outer)(current, parity, chunk + 1)

            if detours:

                @pl.when(carries & (chunk == RELAY_AT))
                def _():
                    received = detour.at[parity]
                    remote(
                        received, received, part_sem.at[0], detour_sem.at[parity], inner_target
                    ).wait_recv()
                    pass_on(current, parity).start()

            over_tiles(chunk, lambda t: update(step, current, other, t))
            if relay:

                @pl.when(has_outer & ((chunk < early) | (chunk >= early + relayed)))
                def _():
                    send_outer(other, 1 - parity, chunk)

                send_inner(other, 1 - parity, chunk)
            else:
                send(other, 1 - parity, chunk)
            return carry

        lax.fori_loop(0, chunks, chunk_body, 0)

    def two_steps(k, carry):
        advance(2 * k, even, odd, 0, False)
        advance(2 * k + 1, odd, even, 1, False)
        return carry

    if helpers:
        advance(0, even, odd, 0, False, True)

        @pl.when(carries)
        def _():
            pass_on(even, 0).wait_send()

        advance(1, odd, even, 1, False)

    lax.fori_loop(1 if helpers else 0, steps // 2 - 1, two_steps, 0)
    advance(steps - 2, even, odd, 0, True)

    def across(t):
        here = tile(PAD + 8 * t)
        value = odd[0, outer_plane, here] * odd[0, outer_halo, here]
        for comp in range(1, 3):
            value = value + odd[comp, outer_plane, here] * odd[comp, outer_halo, here]
        return value

    def returned(first, number, sem):
        where = pl.ds(first * size, number * size)
        return remote(
            product_out.at[where],
            product_in.at[where],
            product_sem.at[0],
            product_sem.at[sem],
            outer_target,
        )

    pieces = [(0, relayed - 1, 1), (relayed - 1, 1, 2)] if relayed > 1 else [(0, relayed, 1)]
    pieces = [piece for piece in pieces if piece[1]]
    if pieces:

        @pl.when(has_outer)
        def _():
            def multiply(chunk, carry):
                received_outer(odd, 1, early + chunk)
                for k in range(tiles):
                    t = chunk * tiles + k
                    product_out[tile(8 * t)] = across(early * tiles + t)
                return carry

            for piece in pieces:
                lax.fori_loop(piece[0], piece[0] + piece[1], multiply, 0)
                returned(*piece).start()

            def follow(chunk, carry):
                send_outer(odd, 1, early + chunk)
                return carry

            lax.fori_loop(0, relayed, follow, 0)

    received_inner(odd, 1)

    def weigh(totals, at, value):
        return tuple(
            totals[i] + fold(pool[(i,) + at] * value) for i in range(2 * pairs)
        )

    def own_part(t, totals):
        def load(comp, plane, shift=0):
            return odd[comp, plane, tile(PAD + 8 * (t + shift))]

        for mid, around in ((inner_plane, (outer_plane, inner_halo)), (outer_plane, (inner_plane,))):
            at = (mid - 1, tile(8 * t))
            value = None
            for comp in range(3):
                centre = load(comp, mid)
                minus_x, plus_x = along_x(load(comp, mid, -1), centre, load(comp, mid, 1))
                minus_y, plus_y = along_y(centre)
                total = load(comp, around[0])
                for plane in around[1:]:
                    total = total + load(comp, plane)
                lap = (total + (minus_x + plus_x)) + ((minus_y + plus_y) - 6.0 * centre)
                value = centre * lap if value is None else value + centre * lap
            value = (shear[at] - prior[at]) + 0.02 * (grad[at] + value)
            grad[at] = value
            totals = weigh(totals, at, value)
        return totals

    totals = lax.fori_loop(
        0,
        rows // 8,
        own_part,
        tuple(jnp.zeros((8, 128), jnp.float32) for _ in range(2 * pairs)),
        unroll=2,
    )
    for i in range(2 * pairs):
        sums[i] = totals[i]

    @pl.when(has_outer)
    def _():
        def add(t, product, totals):
            at = (outer_plane - 1, tile(8 * t))
            value = 0.02 * product
            grad[at] = grad[at] + value
            return weigh(totals, at, value)

        def added(products, start):
            return lambda t, totals: add(start * tiles + t, products[tile(8 * t)], totals)

        totals = tuple(sums[i] for i in range(2 * pairs))
        if relayed:
            totals = lax.fori_loop(0, relayed * tiles, added(product_out, early), totals)

        def direct(chunk, totals):
            received_outer(odd, 1, chunk)
            for k in range(tiles):
                t = chunk * tiles + k
                totals = add(t, across(t), totals)
            return totals

        totals = lax.fori_loop(2 * relayed, chunks, direct, totals)
        for piece in pieces:
            returned(*piece).wait_recv()
            totals = lax.fori_loop(
                piece[0] * tiles,
                (piece[0] + piece[1]) * tiles,
                added(product_in, late),
                totals,
                unroll=tiles,
            )
        for i in range(2 * pairs):
            sums[i] = totals[i]

    line = part[...]
    for i in range(2 * pairs):
        line = jnp.where(place == count + i, whole(sums[i]), line)
    part[...] = line

    def exchange(src, dst, target):
        return remote(src, dst, part_sem.at[0], part_sem.at[1], target)

    for target in range(n):

        @pl.when(me != target)
        def _():
            exchange(part, gathered.at[me], target).start()

    gathered[me] = line

    def close(chunk, carry):
        over_tiles(chunk, lambda t: update(steps - 1, odd, even, t, True))
        return carry

    if relayed > 1:
        lax.fori_loop(2 * relayed + 1, chunks, close, 0)
        after = upper * (relayed + 1)
        lax.fori_loop(after, relayed - 1 + upper * (relayed + 2), close, 0)
    if relayed:

        @pl.when(has_outer)
        def _():
            def arrive(chunk, carry):
                received_outer(odd, 1, late + chunk)
                return carry

            lax.fori_loop(0, relayed, arrive, 0)

    if relayed > 1:
        before = (1 - upper) * (relayed - 1)
        lax.fori_loop(before, 2 * relayed + 1 - upper * relayed, close, 0)
    else:
        lax.fori_loop(0, chunks, close, 0)
    if relayed:

        @pl.when(has_outer)
        def _():
            returned(0, relayed, 1).wait_send()

    sent(even, 0)
    sent(odd, 1)
    arriving = gathered.at[pl.ds(0, n - 1)]
    everything = exchange(arriving, arriving, inner_target)
    everything.wait_recv()
    line = gathered[0]
    for k in range(1, n):
        line = line + gathered[k]
    summed[...] = line
    everything.wait_send()


def publish(
    pairs,
    final,
    grad,
    pool,
    summed,
    final_hbm,
    grad_hbm,
    direction_hbm,
    direction,
    sem,
):
    rows, cols = grad.shape[1], grad.shape[2]
    copies = [
        pltpu.make_async_copy(final, final_hbm, sem.at[0]),
        pltpu.make_async_copy(grad, grad_hbm, sem.at[1]),
    ]
    for copy in copies:
        copy.start()

    place = lax.broadcasted_iota(jnp.int32, (1, 128), 1)
    products = product_pairs(pairs)
    count = len(products)
    where_of = {pair: k for k, pair in enumerate(products)}
    for i in range(2 * pairs):
        where_of[(i, 2 * pairs)] = count + i
    line = summed[...]
    cache = {}

    def inner(a, b):
        key = (min(a, b), max(a, b))
        if key not in cache:
            chosen = jnp.where(place == where_of[key], line, 0.0)
            cache[key] = jnp.sum(chosen, axis=1, keepdims=True)
        return cache[key]

    gradient_at = 2 * pairs
    curvature = [inner(i, pairs + i) for i in range(pairs)]
    alphas = [None] * pairs
    for i in reversed(range(pairs)):
        value = inner(i, gradient_at)
        for j in range(i + 1, pairs):
            value = value - alphas[j] * inner(i, pairs + j)
        alphas[i] = value / curvature[i]
    newest = 2 * pairs - 1
    gamma = curvature[pairs - 1] / inner(newest, newest)
    changes = [-gamma * alphas[i] for i in range(pairs)]
    steps_coef = [None] * pairs
    for i in range(pairs):
        value = gamma * inner(pairs + i, gradient_at)
        for j in range(pairs):
            value = value + changes[j] * inner(pairs + i, pairs + j)
        for j in range(i):
            value = value + steps_coef[j] * inner(j, pairs + i)
        steps_coef[i] = alphas[i] - value / curvature[i]

    def spread(value):
        return -jnp.broadcast_to(value, (8, cols))

    by_grad = spread(gamma)
    by_taken = [spread(value) for value in steps_coef]
    by_change = [spread(value) for value in changes]

    def combine(t, carry):
        for plane in range(2):
            at = (plane, tile(8 * t))
            value = by_grad * grad[at]
            for i in range(pairs):
                value = value + by_taken[i] * pool[(i,) + at]
                value = value + by_change[i] * pool[(pairs + i,) + at]
            direction[at] = value
        return carry

    tiles = rows // 8
    pieces = PIECES
    while tiles % pieces:
        pieces -= 1
    for piece in range(pieces):
        first, count = piece * (tiles // pieces), tiles // pieces
        lax.fori_loop(first, first + count, combine, 0, unroll=True)
        span = pl.ds(8 * first, 8 * count)
        copy = pltpu.make_async_copy(
            direction.at[:, span], direction_hbm.at[:, span], sem.at[2 + piece]
        )
        copy.start()
        copies.append(copy)
    for copy in copies:
        copy.wait()


def on_device(
    n,
    samples,
    field_now,
    field_before,
    lame_lambda,
    shear_modulus,
    density,
    source_field,
    wavelet,
    prior_mean,
    steps_taken,
    grad_change,
):
    comps, depth, rows, cols = field_now.shape
    pairs = steps_taken.shape[0]
    steps = wavelet.shape[0]
    size = chunk_rows(rows)
    chunks = rows // size
    relayed = 3 * chunks // 10
    assist = samples > comps and 8 <= n <= steps + 1 and steps >= 6 and chunks > 4
    helpers = comps - 1 if assist else 0
    f32 = jnp.float32
    state = pltpu.VMEM((comps, depth + 2, rows + 2 * PAD, cols), f32)
    model = pltpu.VMEM((depth, rows, cols), f32)
    returned = pltpu.VMEM((max(relayed, 1) * size, cols), f32)
    dma = pltpu.SemaphoreType.DMA
    anywhere = pl.BlockSpec(memory_space=pltpu.HBM)
    free = pl.BlockSpec(memory_space=pl.ANY)
    in_vmem = pl.BlockSpec(memory_space=pltpu.VMEM)
    results = pl.pallas_call(
        functools.partial(kernel, n, steps, pairs, size, relayed, helpers),
        out_shape=(
            pltpu.VMEM(field_now.shape, f32),
            pltpu.VMEM(lame_lambda.shape, f32),
            pltpu.VMEM((2 * pairs,) + lame_lambda.shape, f32),
            pltpu.VMEM((1, 128), f32),
        ),
        in_specs=[anywhere] * 10,
        out_specs=(in_vmem,) * 4,
        scratch_shapes=[
            state,
            state,
            pltpu.VMEM((4, depth, rows, cols), f32),
            pltpu.VMEM((comps, depth, rows, cols), f32),
            pltpu.SMEM((steps,), f32),
            pltpu.VMEM((2 * pairs, 8, 128), f32),
            pltpu.VMEM((1, 128), f32),
            pltpu.VMEM((n, 1, 128), f32),
            returned,
            returned,
            pltpu.VMEM((1, 2 * size, cols), f32),
            dma((2,)),
            dma((2,)),
            dma((2, chunks)),
            dma((3,)),
            dma((2,)),
            dma((1,)),
            pltpu.SemaphoreType.REGULAR,
        ],
        compiler_params=pltpu.CompilerParams(
            collective_id=0, has_side_effects=True, vmem_limit_bytes=63000000
        ),
    )(
        field_now,
        field_before,
        lame_lambda,
        shear_modulus,
        density,
        source_field,
        wavelet,
        prior_mean,
        steps_taken,
        grad_change,
    )
    return pl.pallas_call(
        functools.partial(publish, pairs),
        out_shape=tuple(
            jax.ShapeDtypeStruct(shape, f32)
            for shape in (field_now.shape, lame_lambda.shape, lame_lambda.shape)
        ),
        in_specs=[in_vmem] * 4,
        out_specs=(free, free, free),
        scratch_shapes=[model, dma((2 + PIECES,))],
        compiler_params=pltpu.CompilerParams(vmem_limit_bytes=4 * 1024 * 1024),
    )(*[pltpu.with_memory_space_constraint(value, pltpu.VMEM) for value in results])


def solution(mesh):
    n = mesh.shape["gz"]
    fields = P("sample", "gz", None, None)
    models = P("gz", "sample", None)
    placed = (
        fields,
        fields,
        models,
        models,
        models,
        fields,
        P("sample"),
        models,
        fields,
        fields,
    )
    return jax.shard_map(
        functools.partial(on_device, n, mesh.shape["sample"]),
        mesh=mesh,
        in_specs=placed,
        out_specs=(fields, models, models),
        check_vma=False,
    )
```
